32 devices in a mesh: groups: 2 (over x), pts: 8 (over z, y), branch: 2 (over core).
Axes of the slice: x: 2, y: 2, z: 4, core: 2. Of those that a mesh axis runs over, the one named last changes fastest.
Arguments:
- point_feat: bfloat16 [2, 65536, 128], P('branch', ('groups', 'pts')), parts along dimension 1, may hold values from -6 to 6
- query_feat: bfloat16 [2, 8192, 768], P('branch', ('groups', 'pts')), parts along dimension 1, may hold values from -640 to 640
- supernode_query: bfloat16 [2, 512, 768], P('branch', ('groups', 'pts')), parts along dimension 1, may hold values from -1000 to 1000
- route_owner: int32 [2, 512, 1], P('branch', 'groups'), parts along dimension 1, may hold values from 0 to 7; in each aligned block of 32 rows (0 to 31, 32 to 63, ..., all dimensions but the last counted through in order) at most 8 rows name the same one
- route_slot: int32 [2, 512], P('branch', 'groups'), parts along dimension 1, may hold values from 0 to 31
- anchor_index: int32 [2, 384], P('branch', 'groups'), parts along dimension 1, may hold values from 0 to 255, as said below
- w_in: bfloat16 [2, 128, 768], P('branch'), may hold values from -0.5 to 0.5
- w_mid: bfloat16 [2, 768, 768], P('branch'), may hold values from -0.21875 to 0.21875
- w_q: bfloat16 [2, 768, 768], P('branch'), may hold values from -0.21875 to 0.21875
- w_kv: bfloat16 [2, 768, 1536], P('branch'), may hold values from -0.21875 to 0.21875
- w_out: bfloat16 [2, 1536, 768], P('branch'), may hold values from -1.25 to 1.25
Outputs:
- result: bfloat16 [2, 8192, 768], P('branch', ('groups', 'pts')), parts along dimension 1
The draws below stay inside these ranges and needn't reach their ends.
There are 2 independent parts, one for each index of `groups`. The reference program is written for one: setup_inputs(seed, part) draws one part's arguments, and reference() takes and returns one part's arrays. A program takes and returns all parts, laid end to end along the dimension named above; an argument that names none is the same for every part. Nothing has to cross between parts.
Inputs may be any that keep to these rules, and one draw needn't show every extreme that they name: `route_owner`: within the rows of one device, at most 8 blocks name one owner, and in every draw some device sends exactly 8 blocks to one owner. `anchor_index`: the 192 entries of each branch are distinct.
All inputs are finite; a program needn't handle non-finite values.
Results may differ from the reference program's by a relative error of at most 0.014.
The reference program's roundings to bfloat16 on the way count: a program that leaves them out, or rounds other values in their place, can miss the bound.
Values may be sent and summed in bfloat16 or wider, within the bound.
No kernel may reach another device: no remote copies, remote signals or barrier semaphores. Data moves between devices by JAX's collectives and lax.ppermute only.
A program may use at most 128 MiB of HBM per device.

```python
import math
import jax
import jax.numpy as jnp
import numpy as np
from jax import lax

D = 768
HEADS = 12
F_IN = 128
BLK = 128
NB_DEV = 32
SN_DEV = 32
ANC_DEV = 24
Q_DEV = 512
CAP = 8
POINTS = 32768
NBLOCKS = 256
N_PTS = 8


def scaled_rows(key, rows):
    base = jax.random.truncated_normal(jax.random.fold_in(key, 11), -4.0, 4.0, (2, rows, D), jnp.float32)
    return base.astype(jnp.bfloat16)


def draw_query_feat(key, part):
    return scaled_rows(jax.random.fold_in(key, 21), Q_DEV * N_PTS)


def draw_supernode_query(key, part):
    return scaled_rows(jax.random.fold_in(key, 31), SN_DEV * N_PTS)


def draw_anchor_index(key, part):
    first = jax.random.permutation(jax.random.fold_in(key, 41), SN_DEV * N_PTS)[:ANC_DEV * N_PTS]
    second = jax.random.permutation(jax.random.fold_in(key, 42), SN_DEV * N_PTS)[:ANC_DEV * N_PTS]
    return jnp.stack([first, second], axis=0).astype(jnp.int32)


def touch_ends(result, key, least, high):
    longest = result.shape.index(max(result.shape))
    spots = []
    for shift in (0, 1):
        where = [jax.random.randint(jax.random.fold_in(key, axis), (), 0, length) for axis, length in enumerate(result.shape)]
        where[longest] = (where[longest] + shift) % result.shape[longest]
        spots.append(tuple(where))
    return result.at[spots[0]].set(least).at[spots[1]].set(high)


def block_levels(own_key, extent, cuts, smallest, largest):
    level, own = 1.0, jax.random.fold_in(own_key, 6)
    for position, parts in cuts:
        draws = jnp.exp(jax.random.uniform(jax.random.fold_in(own, position), (parts,), jnp.float32, smallest / len(cuts), largest / len(cuts)))
        level = level * jnp.repeat(draws, extent[position] // parts).reshape([-1 if axis == position else 1 for axis in range(len(extent))])
    return level


def routed_block(rng, own, number, rows, number_of, top, limit, lean):
    order = jax.random.permutation(rng, number_of)
    crowded, usual = load_shares(number_of, rows * top, limit, lean, True), load_shares(number_of, rows * top, limit, lean, False)
    places = jnp.arange(number_of)

    def named(lengths, turn):
        used = int((lengths > 0).sum())
        fixed = max(1, used // 4)
        moved = fixed + (places - fixed + turn * (used - fixed)) % max(1, number_of - fixed)
        return jnp.zeros((number_of,), jnp.int32).at[order[jnp.where(places < fixed, places, moved)]].set(jnp.asarray(lengths, jnp.int32))

    lengths = jnp.where(number % 4 == 0, named(crowded, number // 4), named(usual, number - number // 4 - 1))
    mixed = jax.random.permutation(jax.random.fold_in(own, 3), number_of)
    donor, receiver = mixed[0:number_of // 2 * 2:2], mixed[1:number_of // 2 * 2:2]
    room = jnp.minimum(lengths[donor] - 1, limit - lengths[receiver]) // 2
    room = jnp.where((donor == order[0]) | (receiver == order[0]) | (lengths[receiver] == 0), 0, jnp.maximum(room, 0))
    moved = jax.random.randint(jax.random.fold_in(own, 4), (number_of // 2,), 0, 1 << 20) % (room + 1)
    lengths = lengths.at[donor].add(-moved).at[receiver].add(moved)
    members = jnp.searchsorted(jnp.cumsum(lengths), jnp.arange(rows * top), side="right").astype(jnp.int32)
    grid = members.reshape(top, rows).T
    grid = grid[jax.random.permutation(jax.random.fold_in(own, 1), rows)]
    turn = jax.random.randint(jax.random.fold_in(own, 2), (rows, 1), 0, top)
    return jnp.take_along_axis(grid, (jnp.arange(top)[None, :] + turn) % top, axis=1)


def load_shares(number_of, total, most, slope, full):
    weights = [(1 << 20) // math.isqrt(rank ** slope) + 1 for rank in range(1, number_of + 1)]
    largest = most if full else min(most, max(-(-total // number_of), total * weights[0] // sum(weights)))
    least = 1 if total - largest >= number_of - 1 else 0
    holding, surplus = [largest] + [least] * (number_of - 1), total - largest - least * (number_of - 1)
    while surplus > 0:
        free = [i for i in range(1, number_of) if holding[i] < largest] or [i for i in range(1, number_of) if holding[i] < most]
        mass, budget = sum([weights[i] for i in free]), surplus
        for i in free:
            extra = min(most - holding[i], max(1, budget * weights[i] // mass), surplus)
            holding[i] = holding[i] + extra
            surplus = surplus - extra
    return np.array(holding)


def centred(own_key, shape, deviation, bound, cuts=(), held_as=jnp.bfloat16):
    values = deviation * jax.random.normal(own_key, shape, jnp.float32)
    if cuts:
        values = values * block_levels(own_key, shape, cuts, -0.22, 0.18)
    return jnp.clip(values, -bound, bound).astype(held_as)


def setup_inputs(seed: int = 0, part: int = 0) -> dict:
    splits = jax.random.split(jax.random.key(seed), 12)
    part_splits = jax.random.split(jax.random.fold_in(splits[11], part), 12)
    point_feat = centred(part_splits[0], (2, POINTS, F_IN), 1.0, 6.0, ((0, 2), (1, 8)))
    query_feat = draw_query_feat(jax.random.fold_in(jax.random.fold_in(splits[11], part), 71), part)
    supernode_query = draw_supernode_query(jax.random.fold_in(jax.random.fold_in(splits[11], part), 71), part)
    route_owner_keys = jax.random.split(jax.random.fold_in(part_splits[3], 1), 2 * NBLOCKS // NB_DEV)
    route_owner_turns = jax.random.permutation(jax.random.fold_in(part_splits[3], 3), 2 * NBLOCKS // NB_DEV)
    route_owner = jax.vmap(lambda own, number: routed_block(jax.random.fold_in(part_splits[3], 2), own, number, NB_DEV, N_PTS, 1, CAP, 2))(route_owner_keys, route_owner_turns).reshape((2, NBLOCKS, 1))
    route_slot = touch_ends(jax.random.randint(part_splits[4], (2, NBLOCKS), 0, SN_DEV), jax.random.fold_in(part_splits[4], 1), 0, SN_DEV - 1).astype(jnp.int32)
    anchor_index = draw_anchor_index(jax.random.fold_in(jax.random.fold_in(splits[11], part), 71), part)
    w_in = centred(splits[6], (2, F_IN, D), F_IN ** -0.5, 0.5, ((0, 2),))
    w_mid = centred(splits[7], (2, D, D), D ** -0.5, 0.21875, ((0, 2),))
    w_q = centred(splits[8], (2, D, D), D ** -0.5, 0.21875, ((0, 2),))
    w_kv = centred(splits[9], (2, D, 2 * D), D ** -0.5, 0.21875, ((0, 2),))
    w_out = centred(splits[10], (2, 2 * D, D), (D // 32) ** -0.5, 1.25, ((0, 2),))
    return dict(point_feat=point_feat, query_feat=query_feat, supernode_query=supernode_query, route_owner=route_owner, route_slot=route_slot, anchor_index=anchor_index, w_in=w_in, w_mid=w_mid, w_q=w_q, w_kv=w_kv, w_out=w_out)


def pool_ref(blocks, queries):
    head_size = D // HEADS
    split_rows = blocks.astype(jnp.float32).reshape(blocks.shape[0], BLK, HEADS, head_size)
    asked_rows = queries.astype(jnp.float32).reshape(queries.shape[0], HEADS, head_size)
    scores = jnp.einsum('nrhe,nhe->nhr', split_rows, asked_rows) / math.sqrt(head_size)
    weights = jax.nn.softmax(scores, axis=-1).astype(jnp.bfloat16).astype(jnp.float32)
    pooled = jnp.einsum('nhr,nrhe->nhe', weights, split_rows)
    return pooled.astype(jnp.bfloat16).reshape(blocks.shape[0], D)

def attend_ref(queries, key_rows, value_rows):
    head_size = D // HEADS
    query_heads = queries.astype(jnp.float32).reshape(queries.shape[0], HEADS, head_size)
    key_heads = key_rows.astype(jnp.float32).reshape(key_rows.shape[0], HEADS, head_size)
    value_heads = value_rows.astype(jnp.float32).reshape(value_rows.shape[0], HEADS, head_size)
    scores = jnp.einsum('qhe,khe->hqk', query_heads, key_heads) / math.sqrt(head_size)
    weights = jax.nn.softmax(scores, axis=-1).astype(jnp.bfloat16).astype(jnp.float32)
    output = jnp.einsum('hqk,khe->qhe', weights, value_heads)
    return output.astype(jnp.bfloat16).reshape(queries.shape[0], D)

def reference(point_feat, query_feat, supernode_query, route_owner, route_slot, anchor_index, w_in, w_mid, w_q, w_kv, w_out):
    anchor_sets = []
    for branch in range(2):
        hidden = jax.nn.gelu(jnp.dot(point_feat[branch], w_in[branch], preferred_element_type=jnp.float32)).astype(jnp.bfloat16)
        encoded = jnp.dot(hidden, w_mid[branch], preferred_element_type=jnp.float32).astype(jnp.bfloat16)
        node_ids = (route_owner[branch, :, 0] * SN_DEV + route_slot[branch]).astype(jnp.int32)
        block_queries = jnp.take(supernode_query[branch], node_ids, axis=0)
        pooled = lax.map(lambda pair: pool_ref(pair[0], pair[1]), (encoded.reshape(N_PTS, NB_DEV, BLK, D), block_queries.reshape(N_PTS, NB_DEV, D)))
        pooled = pooled.reshape(N_PTS * NB_DEV, D)
        all_ids = jnp.arange(SN_DEV * N_PTS, dtype=jnp.int32)
        member = (node_ids[None, :] == all_ids[:, None]).astype(jnp.float32)
        pooled_sum = jnp.dot(member, pooled.astype(jnp.float32), precision=lax.Precision.HIGHEST)
        node_count = lax.optimization_barrier(jnp.sum(member, axis=1))
        combined = supernode_query[branch].astype(jnp.float32) + pooled_sum / jnp.maximum(node_count, 1.0)[:, None]
        node_feat = (combined * lax.rsqrt(lax.optimization_barrier(jnp.mean(combined * combined, axis=1, keepdims=True)) + 1e-06)).astype(jnp.bfloat16)
        anchor_rows = jnp.take(node_feat, anchor_index[branch].astype(jnp.int32), axis=0)
        anchor_sets.append(jnp.dot(anchor_rows, w_kv[branch], preferred_element_type=jnp.float32).astype(jnp.bfloat16))
    outputs = []
    query_count = Q_DEV * N_PTS
    query_step = min(512, Q_DEV)
    for branch in range(2):
        queries = jnp.dot(query_feat[branch], w_q[branch], preferred_element_type=jnp.float32).astype(jnp.bfloat16)
        own_kv = anchor_sets[branch]
        far_kv = anchor_sets[1 - branch]

        def answer(query_rows, own_kv=own_kv, far_kv=far_kv):
            self_out = attend_ref(query_rows, own_kv[:, :D], own_kv[:, D:])
            cross_out = attend_ref(query_rows, far_kv[:, :D], far_kv[:, D:])
            return jnp.concatenate([self_out, cross_out], axis=1)
        joined = lax.map(answer, queries.reshape(query_count // query_step, query_step, D)).reshape(query_count, 2 * D)
        outputs.append(jnp.dot(joined, w_out[branch], preferred_element_type=jnp.float32).astype(jnp.bfloat16))
    return jnp.stack(outputs, axis=0)
```

```python
import math

import jax
import jax.numpy as jnp
from jax import lax
from jax.experimental import pallas as pl
from jax.experimental.pallas import tpu as pltpu
from jax.sharding import PartitionSpec as P

D = 768
HEADS = 12
BLK = 128
HEAD_PAD = 16
MIB = 1 << 20


def call(kernel, out, scratch=(), flops=0, limit=16 * MIB, **kw):
    whole = pl.BlockSpec(memory_space=pltpu.VMEM)

    def run(*args):
        specs = [
            pl.BlockSpec(memory_space=pltpu.SMEM) if a.ndim == 1 else whole for a in args
        ]
        outs = [whole] * len(out) if isinstance(out, (list, tuple)) else whole
        return pl.pallas_call(
            kernel,
            out_shape=out,
            in_specs=specs,
            out_specs=outs,
            scratch_shapes=list(scratch),
            compiler_params=pltpu.CompilerParams(vmem_limit_bytes=limit),
            cost_estimate=pl.CostEstimate(flops=int(flops), bytes_accessed=0, transcendentals=0),
            **kw,
        )(*args)

    return run


def shape(dims, dtype=jnp.bfloat16):
    return jax.ShapeDtypeStruct(tuple(dims), dtype)


def matmul(a, b, dims=((1,), (0,))):
    return lax.dot_general(a, b, (dims, ((), ())), preferred_element_type=jnp.float32)


def spread(blocks, axis):
    count = lax.axis_size(axis)
    copies = jnp.broadcast_to(blocks[None], (count,) + blocks.shape)
    out = lax.all_to_all(copies, axis, split_axis=0, concat_axis=0, tiled=True)
    return out.reshape((count * blocks.shape[0],) + blocks.shape[1:])


def encode_kernel(x_ref, w_in_ref, w_mid_ref, out_ref, hid_ref):
    rows = hid_ref.shape[1]
    steps = x_ref.shape[0] // rows

    def first(step, slot):
        at = pl.ds(pl.multiple_of(step * rows, rows), rows)
        half = matmul(x_ref[at, :], w_in_ref[...])
        inner = half * (2 * math.sqrt(2 / math.pi) + 8 * 0.044715 * math.sqrt(2 / math.pi) * (half * half))
        hid_ref[slot] = (half + half * jnp.tanh(inner)).astype(jnp.bfloat16)

    def second(step, slot):
        at = pl.ds(pl.multiple_of(step * rows, rows), rows)
        out_ref[at, :] = matmul(hid_ref[slot], w_mid_ref[...]).astype(jnp.bfloat16)

    first(0, 0)

    def body(pair, carry):
        step = pair * 2
        first(step + 1, 1)
        second(step, 0)
        first(lax.rem(step + 2, steps), 0)
        second(step + 1, 1)
        return carry

    lax.fori_loop(0, steps // 2, body, 0)


def route_kernel(me_ref, owner_ref, slot_ref, anchor_ref, mine_ref, member_ref, pick_ref, inv_ref, *, nodes_here):
    blocks = owner_ref.shape[1]
    nodes = pick_ref.shape[1]
    anchors = anchor_ref.shape[1]
    nb = mine_ref.shape[0]
    node_ids = (owner_ref[...] * nodes_here + slot_ref[...]).astype(jnp.float32)
    row = lax.broadcasted_iota(jnp.int32, (nb, blocks), 0) + me_ref[0] * nb
    col = lax.broadcasted_iota(jnp.int32, (nb, blocks), 1)
    mine = jnp.sum(jnp.where(row == col, node_ids, 0.0), axis=1, keepdims=True)
    lane = lax.broadcasted_iota(jnp.int32, (nb, nodes), 1).astype(jnp.float32)
    mine_ref[...] = (lane == mine).astype(jnp.bfloat16)
    row = lax.broadcasted_iota(jnp.int32, (anchors, anchors), 0)
    col = lax.broadcasted_iota(jnp.int32, (anchors, anchors), 1)
    ids = anchor_ref[...].astype(jnp.float32)
    wanted = jnp.sum(jnp.where(row == col, ids, 0.0), axis=1, keepdims=True)
    member = (node_ids == wanted).astype(jnp.float32)
    member_ref[...] = member.astype(jnp.bfloat16)
    inv_ref[...] = 1.0 / jnp.maximum(jnp.sum(member, axis=1, keepdims=True), 1.0)
    lane = lax.broadcasted_iota(jnp.int32, (anchors, nodes), 1).astype(jnp.float32)
    pick_ref[...] = (lane == wanted).astype(jnp.bfloat16)


def pool_kernel(mine_ref, nodes_ref, enc_ref, out_ref, qm_ref, score_ref, mix_ref, *, head_size):
    nb, width = out_ref.shape
    rows = enc_ref.shape[0] // nb
    asked = matmul(mine_ref[...], nodes_ref[...]).astype(jnp.bfloat16)
    head = lax.broadcasted_iota(jnp.int32, (HEAD_PAD, width), 0)
    lane = lax.broadcasted_iota(jnp.int32, (HEAD_PAD, width), 1)
    keep = (lane // head_size == head).astype(jnp.float32)
    qm = asked[:, None, :] * keep.astype(jnp.bfloat16)[None]
    qm_ref[...] = qm.reshape(nb * HEAD_PAD, width)
    pad = 2 * HEAD_PAD
    for p in range(nb // 2):
        score_ref[p * pad : (p + 1) * pad, :] = matmul(
            qm_ref[p * pad : (p + 1) * pad, :],
            enc_ref[p * 2 * rows : (p + 1) * 2 * rows, :],
            ((1,), (1,)),
        )
    shape3 = (nb // 2, pad, 2 * rows)
    scores = score_ref[...].reshape(shape3) * (1.0 / math.sqrt(head_size))
    own = lax.broadcasted_iota(jnp.int32, shape3, 1) // HEAD_PAD == lax.broadcasted_iota(
        jnp.int32, shape3, 2
    ) // rows
    top = jnp.max(jnp.where(own, scores, -jnp.inf), axis=2, keepdims=True)
    part = jnp.where(own, jnp.exp(scores - top), 0.0)
    part = part * (1.0 / jnp.sum(part, axis=2, keepdims=True))
    mix_ref[...] = part.astype(jnp.bfloat16).reshape(nb * HEAD_PAD, 2 * rows)
    outs = []
    for p in range(nb // 2):
        mixed = matmul(
            mix_ref[p * pad : (p + 1) * pad, :], enc_ref[p * 2 * rows : (p + 1) * 2 * rows, :]
        )
        outs.append(jnp.sum(mixed.reshape(2, HEAD_PAD, width) * keep[None], axis=1))
    out_ref[...] = jnp.concatenate(outs, axis=0).astype(jnp.bfloat16)


def node_kernel(member_ref, pick_ref, inv_ref, pooled_ref, nodes_ref, w_kv_ref, kv_ref):
    asked = matmul(pick_ref[...], nodes_ref[...])
    value = asked + matmul(member_ref[...], pooled_ref[...]) * inv_ref[...]
    mean = jnp.mean(value * value, axis=1, keepdims=True)
    feat = (value * lax.rsqrt(mean + 1e-06)).astype(jnp.bfloat16)
    kv_ref[...] = matmul(feat, w_kv_ref[...]).astype(jnp.bfloat16)


def query_kernel(feat_ref, w_ref, out_ref, *, scale):
    queries = matmul(feat_ref[...], w_ref[...]) * scale
    out_ref[...] = queries.astype(jnp.bfloat16).T


def attend(q_ref, kv_ref, out_ref, head_size):
    width, _ = q_ref.shape
    anchors = kv_ref.shape[0]
    pair = 2 * head_size
    lane = lax.broadcasted_iota(jnp.int32, (anchors, pair), 1)
    for j in range(width // pair):
        at = slice(j * pair, (j + 1) * pair)
        keys = kv_ref[:, at]
        zero = jnp.zeros_like(keys)
        both = jnp.concatenate(
            [jnp.where(lane < head_size, keys, zero), jnp.where(lane >= head_size, keys, zero)], axis=0
        )
        scores = matmul(both, q_ref[at, :])
        values = kv_ref[:, width + j * pair : width + (j + 1) * pair].T
        for h in range(2):
            part = scores[h * anchors : (h + 1) * anchors]
            part = jnp.exp(part - jnp.max(part, axis=0, keepdims=True))
            part = part * (1.0 / jnp.sum(part, axis=0, keepdims=True))
            got = matmul(values[h * head_size : (h + 1) * head_size], part.astype(jnp.bfloat16))
            base = j * pair + h * head_size
            out_ref[base : base + head_size, :] = got.astype(jnp.bfloat16)


def self_kernel(q_ref, kv_ref, w_ref, out_ref, mid_ref, *, head_size):
    attend(q_ref, kv_ref, mid_ref, head_size)
    out_ref[...] = matmul(mid_ref[...].T, w_ref[...])


def cross_kernel(q_ref, kv_ref, w_ref, own_ref, out_ref, mid_ref, *, head_size):
    attend(q_ref, kv_ref, mid_ref, head_size)
    out_ref[...] = (own_ref[...] + matmul(mid_ref[...].T, w_ref[...])).astype(jnp.bfloat16)


def per_device(
    point_feat,
    query_feat,
    supernode_query,
    route_owner,
    route_slot,
    anchor_index,
    w_in,
    w_mid,
    w_q,
    w_kv,
    w_out,
):
    import functools

    head_size = D // HEADS
    shard_count = lax.axis_size("pts")
    me = lax.axis_index("pts").astype(jnp.int32).reshape(1)
    points = point_feat[0]
    nblocks = points.shape[0] // BLK
    own = supernode_query[0]
    nodes_here, width = own.shape
    owners = route_owner.reshape(1, -1)
    blocks = owners.shape[1]
    nodes = nodes_here * shard_count
    anchors = anchor_index.shape[1]
    query_count = query_feat.shape[1]

    all_nodes = spread(own, "pts")
    rows = 512
    encoded = call(
        encode_kernel,
        shape(points.shape[:1] + (width,)),
        [pltpu.VMEM((2, rows, width), jnp.bfloat16)],
        flops=2 * points.shape[0] * width * (width + points.shape[1]),
    )(points, w_in[0] * jnp.bfloat16(0.5), w_mid[0])
    mine, member, pick, inv = call(
        functools.partial(route_kernel, nodes_here=nodes_here),
        [
            shape((nblocks, nodes)),
            shape((anchors, blocks)),
            shape((anchors, nodes)),
            shape((anchors, 1), jnp.float32),
        ],
        flops=1e8,
    )(me, owners, route_slot, anchor_index)
    pooled = call(
        functools.partial(pool_kernel, head_size=head_size),
        shape((nblocks, width)),
        [
            pltpu.VMEM((nblocks * HEAD_PAD, width), jnp.bfloat16),
            pltpu.VMEM((nblocks * HEAD_PAD, 2 * BLK), jnp.float32),
            pltpu.VMEM((nblocks * HEAD_PAD, 2 * BLK), jnp.bfloat16),
        ],
        flops=3e9,
    )(mine, all_nodes, encoded)
    all_pooled = spread(pooled, "pts")
    queries = call(
        functools.partial(query_kernel, scale=1.0 / math.sqrt(head_size)),
        shape((width, query_count)),
        flops=2 * query_count * width * width,
    )(query_feat[0], w_q[0])
    anchor_kv = call(node_kernel, shape((anchors, 2 * width)), flops=1e9)(
        member, pick, inv, all_pooled, all_nodes, w_kv[0]
    )
    partner_kv = lax.ppermute(anchor_kv, "branch", [(0, 1), (1, 0)])
    mid = [pltpu.VMEM((width, query_count), jnp.bfloat16)]
    self_part = call(
        functools.partial(self_kernel, head_size=head_size),
        shape((query_count, width), jnp.float32),
        mid,
        flops=3e9,
    )(queries, anchor_kv, w_out[0, :width])
    result = call(
        functools.partial(cross_kernel, head_size=head_size),
        shape((query_count, width)),
        mid,
        flops=3e9,
    )(queries, partner_kv, w_out[0, width:], self_part)
    return result[None]


def solution(mesh):
    return jax.shard_map(
        per_device,
        mesh=mesh,
        in_specs=(
            P("branch", ("groups", "pts"), None),
            P("branch", ("groups", "pts"), None),
            P("branch", ("groups", "pts"), None),
            P("branch", "groups", None),
            P("branch", "groups"),
            P("branch", "groups"),
            P("branch", None, None),
            P("branch", None, None),
            P("branch", None, None),
            P("branch", None, None),
            P("branch", None, None),
        ),
        out_specs=P("branch", ("groups", "pts"), None),
        check_vma=False,
    )
```

```python
import math

import jax
import jax.numpy as jnp
from jax import lax
from jax.experimental import pallas as pl
from jax.experimental.pallas import tpu as pltpu
from jax.sharding import PartitionSpec as P

D = 768
HEADS = 12
BLK = 128
HEAD_PAD = 16
MIB = 1 << 20


def call(kernel, out, scratch=(), flops=0, limit=16 * MIB, **kw):
    whole = pl.BlockSpec(memory_space=pltpu.VMEM)

    def run(*args):
        specs = [
            pl.BlockSpec(memory_space=pltpu.SMEM) if a.ndim == 1 else whole for a in args
        ]
        outs = [whole] * len(out) if isinstance(out, (list, tuple)) else whole
        return pl.pallas_call(
            kernel,
            out_shape=out,
            in_specs=specs,
            out_specs=outs,
            scratch_shapes=list(scratch),
            compiler_params=pltpu.CompilerParams(vmem_limit_bytes=limit),
            cost_estimate=pl.CostEstimate(flops=int(flops), bytes_accessed=0, transcendentals=0),
            **kw,
        )(*args)

    return run


def shape(dims, dtype=jnp.bfloat16):
    return jax.ShapeDtypeStruct(tuple(dims), dtype)


def matmul(a, b, dims=((1,), (0,))):
    return lax.dot_general(a, b, (dims, ((), ())), preferred_element_type=jnp.float32)


def swapped(block, mask):
    count = lax.axis_size("pts")
    return lax.ppermute(block, "pts", [(i, i ^ mask) for i in range(count)])


def masks(count):
    assert count >= 4 and count & (count - 1) == 0, count
    return [1 << b for b in reversed(range(count.bit_length() - 1))]


def after(value, *others):
    return lax.optimization_barrier((value,) + others)[0]


def placed(me_ref, count, dims, axis, inner):
    lane = lax.broadcasted_iota(jnp.int32, dims, axis)
    place = lane // inner
    source = me_ref[0]
    for s, mask in enumerate(masks(count)):
        source = source ^ (((place >> s) & 1) * mask)
    return source * inner + lane % inner


def column(row):
    n = row.shape[1]
    at = lax.broadcasted_iota(jnp.int32, (n, n), 0) == lax.broadcasted_iota(jnp.int32, (n, n), 1)
    return jnp.sum(jnp.where(at, row, 0.0), axis=1, keepdims=True)


def encode_kernel(x_ref, w_in_ref, w_mid_ref, out_ref, hid_ref, *, base):
    rows = hid_ref.shape[1]
    steps = out_ref.shape[0] // rows
    root = math.sqrt(2 / math.pi)

    def first(step):
        at = base + step * rows
        half = matmul(x_ref[at : at + rows, :], w_in_ref[...])
        inner = half * (2 * root + 8 * 0.044715 * root * (half * half))
        hid_ref[step % 2] = (half + half * jnp.tanh(inner)).astype(jnp.bfloat16)

    first(0)
    for step in range(steps):
        if step + 1 < steps:
            first(step + 1)
        out_ref[step * rows : (step + 1) * rows, :] = matmul(
            hid_ref[step % 2], w_mid_ref[...]
        ).astype(jnp.bfloat16)


def pool_kernel(me_ref, owner_ref, slot_ref, held_ref, *refs, head_size, nodes_here):
    *enc_refs, out_ref, qm_ref, score_ref, mix_ref = refs
    nb, width = out_ref.shape
    nodes = held_ref.shape[0]
    rows = sum(e.shape[0] for e in enc_refs) // nb
    pairs = [(e, i * 2 * rows) for e in enc_refs for i in range(e.shape[0] // (2 * rows))]
    blocks = owner_ref.shape[1]
    node_ids = (owner_ref[...] * nodes_here + slot_ref[...]).astype(jnp.float32)
    row = lax.broadcasted_iota(jnp.int32, (nb, blocks), 0) + me_ref[0] * nb
    col = lax.broadcasted_iota(jnp.int32, (nb, blocks), 1)
    wanted = jnp.sum(jnp.where(row == col, node_ids, 0.0), axis=1, keepdims=True)
    there = placed(me_ref, nodes // nodes_here, (nb, nodes), 1, nodes_here).astype(jnp.float32)
    mine = (there == wanted).astype(jnp.float32).astype(jnp.bfloat16)
    asked = matmul(mine, held_ref[...]).astype(jnp.bfloat16)
    head = lax.broadcasted_iota(jnp.int32, (HEAD_PAD, width), 0)
    lane = lax.broadcasted_iota(jnp.int32, (HEAD_PAD, width), 1)
    keep = (lane // head_size == head).astype(jnp.float32)
    qm = asked[:, None, :] * keep.astype(jnp.bfloat16)[None]
    qm_ref[...] = qm.reshape(nb * HEAD_PAD, width)
    pad = 2 * HEAD_PAD
    for p, (enc_ref, at) in enumerate(pairs):
        score_ref[p * pad : (p + 1) * pad, :] = matmul(
            qm_ref[p * pad : (p + 1) * pad, :], enc_ref[at : at + 2 * rows, :], ((1,), (1,))
        )
    shape3 = (nb // 2, pad, 2 * rows)
    scores = score_ref[...].reshape(shape3) * (1.0 / math.sqrt(head_size))
    own = lax.broadcasted_iota(jnp.int32, shape3, 1) // HEAD_PAD == lax.broadcasted_iota(
        jnp.int32, shape3, 2
    ) // rows
    top = jnp.max(jnp.where(own, scores, -jnp.inf), axis=2, keepdims=True)
    part = jnp.where(own, jnp.exp(scores - top), 0.0)
    part = part * (1.0 / jnp.sum(part, axis=2, keepdims=True))
    mix_ref[...] = part.astype(jnp.bfloat16).reshape(nb * HEAD_PAD, 2 * rows)
    outs = []
    for p, (enc_ref, at) in enumerate(pairs):
        mixed = matmul(mix_ref[p * pad : (p + 1) * pad, :], enc_ref[at : at + 2 * rows, :])
        outs.append(jnp.sum(mixed.reshape(2, HEAD_PAD, width) * keep[None], axis=1))
    out_ref[...] = jnp.concatenate(outs, axis=0).astype(jnp.bfloat16)


def query_kernel(
    me_ref,
    owner_ref,
    slot_ref,
    anchor_ref,
    held_ref,
    feat_ref,
    w_ref,
    out_ref,
    asked_ref,
    member_ref,
    inv_ref,
    *,
    scale,
    nodes_here,
):
    blocks = owner_ref.shape[1]
    nodes = held_ref.shape[0]
    anchors = anchor_ref.shape[1]
    count = nodes // nodes_here
    queries = matmul(feat_ref[...], w_ref[...]) * scale
    out_ref[...] = queries.astype(jnp.bfloat16).T
    node_ids = (owner_ref[...] * nodes_here + slot_ref[...]).astype(jnp.float32)
    wanted = column(anchor_ref[...].astype(jnp.float32))
    member = (node_ids == wanted).astype(jnp.float32)
    inv_ref[...] = 1.0 / jnp.maximum(jnp.sum(member, axis=1, keepdims=True), 1.0)
    row = lax.broadcasted_iota(jnp.int32, (blocks, blocks), 0)
    moved = row == placed(me_ref, count, (blocks, blocks), 1, blocks // count)
    moved = moved.astype(jnp.float32).astype(jnp.bfloat16)
    member_ref[...] = matmul(member.astype(jnp.bfloat16), moved).astype(jnp.bfloat16)
    there = placed(me_ref, count, (anchors, nodes), 1, nodes_here).astype(jnp.float32)
    pick = (there == wanted).astype(jnp.float32).astype(jnp.bfloat16)
    asked_ref[...] = matmul(pick, held_ref[...])


def node_kernel(member_ref, inv_ref, asked_ref, pooled_ref, w_kv_ref, kv_ref):
    value = asked_ref[...] + matmul(member_ref[...], pooled_ref[...]) * inv_ref[...]
    mean = jnp.mean(value * value, axis=1, keepdims=True)
    feat = (value * lax.rsqrt(mean + 1e-06)).astype(jnp.bfloat16)
    kv_ref[...] = matmul(feat, w_kv_ref[...]).astype(jnp.bfloat16)


def attend(q_ref, kv_ref, out_ref, head_size):
    width, _ = q_ref.shape
    anchors = kv_ref.shape[0]
    pair = 2 * head_size
    lane = lax.broadcasted_iota(jnp.int32, (anchors, pair), 1)
    for j in range(width // pair):
        at = slice(j * pair, (j + 1) * pair)
        keys = kv_ref[:, at]
        zero = jnp.zeros_like(keys)
        both = jnp.concatenate(
            [jnp.where(lane < head_size, keys, zero), jnp.where(lane >= head_size, keys, zero)], axis=0
        )
        scores = matmul(both, q_ref[at, :])
        values = kv_ref[:, width + j * pair : width + (j + 1) * pair].T
        ones = jnp.ones((HEAD_PAD, anchors), jnp.bfloat16)
        for h in range(2):
            part = scores[h * anchors : (h + 1) * anchors]
            part = jnp.exp2(part - jnp.max(part, axis=0, keepdims=True)).astype(jnp.bfloat16)
            left = jnp.concatenate([values[h * head_size : (h + 1) * head_size], ones], axis=0)
            got = matmul(left, part)
            got = got[:head_size] * (1.0 / got[head_size : head_size + 1])
            base = j * pair + h * head_size
            out_ref[base : base + head_size, :] = got.astype(jnp.bfloat16)


def self_kernel(q_ref, kv_ref, w_ref, out_ref, mid_ref, *, head_size):
    attend(q_ref, kv_ref, mid_ref, head_size)
    width = mid_ref.shape[0]
    out_ref[...] = matmul(mid_ref[...].T, w_ref[:width, :])


def cross_kernel(q_ref, kv_ref, w_ref, own_ref, out_ref, mid_ref, *, head_size):
    attend(q_ref, kv_ref, mid_ref, head_size)
    width = mid_ref.shape[0]
    out_ref[...] = (own_ref[...] + matmul(mid_ref[...].T, w_ref[width:, :])).astype(jnp.bfloat16)


def per_device(
    point_feat,
    query_feat,
    supernode_query,
    route_owner,
    route_slot,
    anchor_index,
    w_in,
    w_mid,
    w_q,
    w_kv,
    w_out,
):
    import functools

    head_size = D // HEADS
    shard_count = lax.axis_size("pts")
    me = lax.axis_index("pts").astype(jnp.int32).reshape(1)
    points = point_feat[0]
    nblocks = points.shape[0] // BLK
    own = supernode_query[0]
    nodes_here, width = own.shape
    owners = route_owner.reshape(1, -1)
    blocks = owners.shape[1]
    nodes = nodes_here * shard_count
    anchors = anchor_index.shape[1]
    query_count = query_feat.shape[1]

    bits = masks(shard_count)
    rows = 2 * BLK
    w_half = w_in[0] * jnp.bfloat16(0.5)
    log_e = 1.0 / math.log(2.0)

    def encode(points, begin, end):
        return call(
            functools.partial(encode_kernel, base=begin),
            shape((end - begin, width)),
            [pltpu.VMEM((2, rows, width), jnp.bfloat16)],
            flops=2 * (end - begin) * width * (width + points.shape[1]),
        )(points, w_half, w_mid[0])

    def pieces(stages):
        pairs = nblocks // 2
        cuts = [rows * (pairs * s // stages) for s in range(stages + 1)]
        return list(zip(cuts[:-1], cuts[1:]))

    stages = bits[:-2] + [bits[-2:]]
    held, encoded = own, []
    for stage, (begin, end) in zip(stages, pieces(len(stages))):
        last = isinstance(stage, list)
        got = [swapped(held, m) for m in (stage + [sum(stage)] if last else [stage])]
        encoded.append(encode(after(points, held) if encoded else points, begin, end))
        got = [after(g, encoded[-1]) for g in got]
        held = jnp.concatenate([held] + got, axis=0)
    all_nodes = held
    pooled = call(
        functools.partial(pool_kernel, head_size=head_size, nodes_here=nodes_here),
        shape((nblocks, width)),
        [
            pltpu.VMEM((nblocks * HEAD_PAD, width), jnp.bfloat16),
            pltpu.VMEM((nblocks * HEAD_PAD, 2 * BLK), jnp.float32),
            pltpu.VMEM((nblocks * HEAD_PAD, 2 * BLK), jnp.bfloat16),
        ],
        flops=3e9,
    )(me, owners, route_slot, all_nodes, *encoded)
    held = pooled
    for stage in stages:
        last = isinstance(stage, list)
        got = [swapped(held, m) for m in (stage + [sum(stage)] if last else [stage])]
        held = jnp.concatenate([held] + got, axis=0)
    all_pooled = held
    queries, asked, member, inv = call(
        functools.partial(query_kernel, scale=log_e / math.sqrt(head_size), nodes_here=nodes_here),
        [
            shape((width, query_count)),
            shape((anchors, width), jnp.float32),
            shape((anchors, blocks)),
            shape((anchors, 1), jnp.float32),
        ],
        flops=2 * query_count * width * width,
        limit=24 * MIB,
    )(me, owners, route_slot, anchor_index, after(all_nodes, pooled), query_feat[0], w_q[0])
    anchor_kv = call(node_kernel, shape((anchors, 2 * width)), flops=1e9)(
        member, inv, asked, all_pooled, w_kv[0]
    )
    partner_kv = lax.ppermute(anchor_kv, "branch", [(0, 1), (1, 0)])
    mid = [pltpu.VMEM((width, query_count), jnp.bfloat16)]
    self_part = call(
        functools.partial(self_kernel, head_size=head_size),
        shape((query_count, width), jnp.float32),
        mid,
        flops=3e9,
    )(queries, anchor_kv, w_out[0])
    result = call(
        functools.partial(cross_kernel, head_size=head_size),
        shape((query_count, width)),
        mid,
        flops=3e9,
    )(queries, partner_kv, w_out[0], self_part)
    return result[None]


def solution(mesh):
    return jax.shard_map(
        per_device,
        mesh=mesh,
        in_specs=(
            P("branch", ("groups", "pts"), None),
            P("branch", ("groups", "pts"), None),
            P("branch", ("groups", "pts"), None),
            P("branch", "groups", None),
            P("branch", "groups"),
            P("branch", "groups"),
            P("branch", None, None),
            P("branch", None, None),
            P("branch", None, None),
            P("branch", None, None),
            P("branch", None, None),
        ),
        out_specs=P("branch", ("groups", "pts"), None),
        check_vma=False,
    )
```

```python
import math

import jax
import jax.numpy as jnp
from jax import lax
from jax.experimental import pallas as pl
from jax.experimental.pallas import tpu as pltpu
from jax.sharding import PartitionSpec as P

D = 768
HEADS = 12
BLK = 128
HEAD_PAD = 16
MIB = 1 << 20


def call(kernel, out, scratch=(), flops=0, limit=16 * MIB, far=(), far_out=False, **kw):
    whole = pl.BlockSpec(memory_space=pltpu.VMEM)
    hbm = pl.BlockSpec(memory_space=pltpu.HBM)

    def run(*args):
        specs = [
            pl.BlockSpec(memory_space=pltpu.SMEM) if a.ndim == 1 else hbm if i in far else whole
            for i, a in enumerate(args)
        ]
        whole_out = hbm if far_out else whole
        outs = [whole_out] * len(out) if isinstance(out, (list, tuple)) else whole_out
        return pl.pallas_call(
            kernel,
            out_shape=out,
            in_specs=specs,
            out_specs=outs,
            scratch_shapes=list(scratch),
            compiler_params=pltpu.CompilerParams(vmem_limit_bytes=limit),
            cost_estimate=pl.CostEstimate(flops=int(flops), bytes_accessed=0, transcendentals=0),
            **kw,
        )(*args)

    return run


def shape(dims, dtype=jnp.bfloat16):
    return jax.ShapeDtypeStruct(tuple(dims), dtype)


def matmul(a, b, dims=((1,), (0,))):
    return lax.dot_general(a, b, (dims, ((), ())), preferred_element_type=jnp.float32)


def swapped(block, mask):
    count = lax.axis_size("pts")
    return lax.ppermute(block, "pts", [(i, i ^ mask) for i in range(count)])


def masks(count):
    assert count >= 8 and count & (count - 1) == 0, count
    return [1 << b for b in reversed(range(count.bit_length() - 1))]


def after(value, *others):
    return lax.optimization_barrier((value,) + others)[0]


def placed(me_ref, count, dims, axis, inner):
    lane = lax.broadcasted_iota(jnp.int32, dims, axis)
    place = lane // inner
    source = me_ref[0]
    for s, mask in enumerate(masks(count)):
        source = source ^ (((place >> s) & 1) * mask)
    return source * inner + lane % inner


def column(row):
    n = row.shape[1]
    at = lax.broadcasted_iota(jnp.int32, (n, n), 0) == lax.broadcasted_iota(jnp.int32, (n, n), 1)
    return jnp.sum(jnp.where(at, row, 0.0), axis=1, keepdims=True)


def encode_rows(rows, steps, load, w_half, w_mid_ref, hid_ref, store):
    root = math.sqrt(2 / math.pi)

    def first(step):
        half = matmul(load(step), w_half())
        inner = half * (2 * root + 8 * 0.044715 * root * (half * half))
        hid_ref[step % 2] = (half + half * jnp.tanh(inner)).astype(jnp.bfloat16)

    first(0)
    for step in range(steps):
        if step + 1 < steps:
            first(step + 1)
        store(step, matmul(hid_ref[step % 2], w_mid_ref[...]).astype(jnp.bfloat16))


def encode_kernel(x_ref, w_in_ref, w_mid_ref, out_ref, hid_ref, half_ref, *, base):
    rows = hid_ref.shape[1]
    half_ref[...] = w_in_ref[...] * jnp.bfloat16(0.5)

    def load(step):
        return x_ref[base + step * rows : base + (step + 1) * rows, :]

    def store(step, value):
        out_ref[step * rows : (step + 1) * rows, :] = value

    encode_rows(
        rows, out_ref.shape[0] // rows, load, lambda: half_ref[...], w_mid_ref, hid_ref, store
    )


def encode_far_kernel(
    x_far, w_in_far, w_mid_far, out_far, hid_ref, half_ref, x_ref, w_in_ref, w_mid_ref, out_ref, in_sem, out_sem, *, base
):
    rows = hid_ref.shape[1]
    steps = out_far.shape[0] // rows
    ins = [
        pltpu.make_async_copy(w_in_far, w_in_ref, in_sem.at[0]),
        pltpu.make_async_copy(x_far.at[pl.ds(base, out_far.shape[0])], x_ref, in_sem.at[1]),
        pltpu.make_async_copy(w_mid_far, w_mid_ref, in_sem.at[2]),
    ]
    for copy in ins:
        copy.start()
    ins[0].wait()
    half_ref[...] = w_in_ref[...] * jnp.bfloat16(0.5)
    ins[1].wait()
    ins[2].wait()
    outs = []

    def load(step):
        return x_ref[step * rows : (step + 1) * rows, :]

    def store(step, value):
        at = pl.ds(step * rows, rows)
        out_ref[at, :] = value
        outs.append(pltpu.make_async_copy(out_ref.at[at], out_far.at[at], out_sem.at[step]))
        outs[step].start()

    encode_rows(rows, steps, load, lambda: half_ref[...], w_mid_ref, hid_ref, store)
    for copy in outs:
        copy.wait()


def pool_kernel(me_ref, owner_ref, slot_ref, held_ref, *refs, head_size, nodes_here):
    *enc_refs, out_ref, qm_ref, score_ref, mix_ref = refs
    nb, width = out_ref.shape
    nodes = held_ref.shape[0]
    rows = sum(e.shape[0] for e in enc_refs) // nb
    pairs = [(e, i * 2 * rows) for e in enc_refs for i in range(e.shape[0] // (2 * rows))]
    blocks = owner_ref.shape[1]
    node_ids = (owner_ref[...] * nodes_here + slot_ref[...]).astype(jnp.float32)
    row = lax.broadcasted_iota(jnp.int32, (nb, blocks), 0) + me_ref[0] * nb
    col = lax.broadcasted_iota(jnp.int32, (nb, blocks), 1)
    wanted = jnp.sum(jnp.where(row == col, node_ids, 0.0), axis=1, keepdims=True)
    there = placed(me_ref, nodes // nodes_here, (nb, nodes), 1, nodes_here).astype(jnp.float32)
    mine = (there == wanted).astype(jnp.float32).astype(jnp.bfloat16)
    asked = matmul(mine, held_ref[...]).astype(jnp.bfloat16)
    head = lax.broadcasted_iota(jnp.int32, (HEAD_PAD, width), 0)
    lane = lax.broadcasted_iota(jnp.int32, (HEAD_PAD, width), 1)
    keep = (lane // head_size == head).astype(jnp.float32)
    qm = asked[:, None, :] * keep.astype(jnp.bfloat16)[None]
    qm_ref[...] = qm.reshape(nb * HEAD_PAD, width)
    pad = 2 * HEAD_PAD
    for p, (enc_ref, at) in enumerate(pairs):
        score_ref[p * pad : (p + 1) * pad, :] = matmul(
            qm_ref[p * pad : (p + 1) * pad, :], enc_ref[at : at + 2 * rows, :], ((1,), (1,))
        )
    shape3 = (nb // 2, pad, 2 * rows)
    scores = score_ref[...].reshape(shape3) * (1.0 / math.sqrt(head_size))
    own = lax.broadcasted_iota(jnp.int32, shape3, 1) // HEAD_PAD == lax.broadcasted_iota(
        jnp.int32, shape3, 2
    ) // rows
    top = jnp.max(jnp.where(own, scores, -jnp.inf), axis=2, keepdims=True)
    part = jnp.where(own, jnp.exp(scores - top), 0.0)
    part = part * (1.0 / jnp.sum(part, axis=2, keepdims=True))
    mix_ref[...] = part.astype(jnp.bfloat16).reshape(nb * HEAD_PAD, 2 * rows)
    outs = []
    for p, (enc_ref, at) in enumerate(pairs):
        mixed = matmul(mix_ref[p * pad : (p + 1) * pad, :], enc_ref[at : at + 2 * rows, :])
        outs.append(jnp.sum(mixed.reshape(2, HEAD_PAD, width) * keep[None], axis=1))
    out_ref[...] = jnp.concatenate(outs, axis=0).astype(jnp.bfloat16)


def query_kernel(
    me_ref,
    owner_ref,
    slot_ref,
    anchor_ref,
    held_ref,
    feat_ref,
    w_ref,
    out_ref,
    asked_ref,
    member_ref,
    inv_ref,
    *,
    scale,
    nodes_here,
):
    blocks = owner_ref.shape[1]
    nodes = held_ref.shape[0]
    anchors = anchor_ref.shape[1]
    count = nodes // nodes_here
    queries = matmul(feat_ref[...], w_ref[...]) * scale
    out_ref[...] = queries.astype(jnp.bfloat16).T
    node_ids = (owner_ref[...] * nodes_here + slot_ref[...]).astype(jnp.float32)
    wanted = column(anchor_ref[...].astype(jnp.float32))
    member = (node_ids == wanted).astype(jnp.float32)
    inv_ref[...] = 1.0 / jnp.maximum(jnp.sum(member, axis=1, keepdims=True), 1.0)
    row = lax.broadcasted_iota(jnp.int32, (blocks, blocks), 0)
    moved = row == placed(me_ref, count, (blocks, blocks), 1, blocks // count)
    moved = moved.astype(jnp.float32).astype(jnp.bfloat16)
    member_ref[...] = matmul(member.astype(jnp.bfloat16), moved).astype(jnp.bfloat16)
    there = placed(me_ref, count, (anchors, nodes), 1, nodes_here).astype(jnp.float32)
    pick = (there == wanted).astype(jnp.float32).astype(jnp.bfloat16)
    asked_ref[...] = matmul(pick, held_ref[...])


def node_kernel(member_ref, inv_ref, asked_ref, pooled_ref, w_kv_ref, kv_ref):
    value = asked_ref[...] + matmul(member_ref[...], pooled_ref[...]) * inv_ref[...]
    mean = jnp.mean(value * value, axis=1, keepdims=True)
    feat = (value * lax.rsqrt(mean + 1e-06)).astype(jnp.bfloat16)
    kv_ref[...] = matmul(feat, w_kv_ref[...]).astype(jnp.bfloat16)


def attend(q_ref, kv_ref, out_ref, head_size):
    width, _ = q_ref.shape
    anchors = kv_ref.shape[0]
    pair = 2 * head_size
    lane = lax.broadcasted_iota(jnp.int32, (anchors, pair), 1)
    for j in range(width // pair):
        at = slice(j * pair, (j + 1) * pair)
        keys = kv_ref[:, at]
        zero = jnp.zeros_like(keys)
        both = jnp.concatenate(
            [jnp.where(lane < head_size, keys, zero), jnp.where(lane >= head_size, keys, zero)], axis=0
        )
        scores = matmul(both, q_ref[at, :])
        values = kv_ref[:, width + j * pair : width + (j + 1) * pair].T
        ones = jnp.ones((HEAD_PAD, anchors), jnp.bfloat16)
        for h in range(2):
            part = scores[h * anchors : (h + 1) * anchors]
            part = jnp.exp2(part - jnp.max(part, axis=0, keepdims=True)).astype(jnp.bfloat16)
            left = jnp.concatenate([values[h * head_size : (h + 1) * head_size], ones], axis=0)
            got = matmul(left, part)
            got = got[:head_size] * (1.0 / got[head_size : head_size + 1])
            base = j * pair + h * head_size
            out_ref[base : base + head_size, :] = got.astype(jnp.bfloat16)


def self_kernel(q_ref, kv_ref, w_ref, out_ref, mid_ref, *, head_size):
    attend(q_ref, kv_ref, mid_ref, head_size)
    width = mid_ref.shape[0]
    out_ref[...] = matmul(mid_ref[...].T, w_ref[:width, :])


def cross_kernel(q_ref, kv_ref, w_ref, own_ref, out_ref, mid_ref, *, head_size):
    attend(q_ref, kv_ref, mid_ref, head_size)
    width = mid_ref.shape[0]
    out_ref[...] = (own_ref[...] + matmul(mid_ref[...].T, w_ref[width:, :])).astype(jnp.bfloat16)


def per_device(
    point_feat,
    query_feat,
    supernode_query,
    route_owner,
    route_slot,
    anchor_index,
    w_in,
    w_mid,
    w_q,
    w_kv,
    w_out,
):
    import functools

    head_size = D // HEADS
    shard_count = lax.axis_size("pts")
    me = lax.axis_index("pts").astype(jnp.int32).reshape(1)
    points = point_feat[0]
    nblocks = points.shape[0] // BLK
    own = supernode_query[0]
    nodes_here, width = own.shape
    owners = route_owner.reshape(1, -1)
    blocks = owners.shape[1]
    nodes = nodes_here * shard_count
    anchors = anchor_index.shape[1]
    query_count = query_feat.shape[1]

    bits = masks(shard_count)
    rows = 2 * BLK
    log_e = 1.0 / math.log(2.0)

    def encode(points, begin, end, near):
        scratch = [
            pltpu.VMEM((2, rows, width), jnp.bfloat16),
            pltpu.VMEM(w_in.shape[1:], jnp.bfloat16),
        ]
        if not near:
            scratch += [
                pltpu.VMEM((end - begin, points.shape[1]), jnp.bfloat16),
                pltpu.VMEM(w_in.shape[1:], jnp.bfloat16),
                pltpu.VMEM(w_mid.shape[1:], jnp.bfloat16),
                pltpu.VMEM((end - begin, width), jnp.bfloat16),
                pltpu.SemaphoreType.DMA((3,)),
                pltpu.SemaphoreType.DMA(((end - begin) // rows,)),
            ]
        return call(
            functools.partial(encode_kernel if near else encode_far_kernel, base=begin),
            shape((end - begin, width)),
            scratch,
            flops=2 * (end - begin) * width * (width + points.shape[1]),
            far=() if near else (0, 1, 2),
            far_out=not near,
            limit=16 * MIB if near else 60 * MIB,
        )(points, w_in[0], w_mid[0])

    def pieces(stages):
        pairs = nblocks // 2
        cuts = [rows * (pairs * s // stages) for s in range(stages + 1)]
        return list(zip(cuts[:-1], cuts[1:]))

    stages = bits[:-2] + [bits[-2:]]
    held, encoded = own, []
    for stage, (begin, end) in zip(stages, pieces(len(stages))):
        last = isinstance(stage, list)
        got = [swapped(held, m) for m in (stage + [sum(stage)] if last else [stage])]
        encoded.append(encode(after(points, held) if encoded else points, begin, end, last))
        got = [after(g, encoded[-1]) for g in got]
        held = jnp.concatenate([held] + got, axis=0)
    all_nodes = held
    pooled = call(
        functools.partial(pool_kernel, head_size=head_size, nodes_here=nodes_here),
        shape((nblocks, width)),
        [
            pltpu.VMEM((nblocks * HEAD_PAD, width), jnp.bfloat16),
            pltpu.VMEM((nblocks * HEAD_PAD, 2 * BLK), jnp.float32),
            pltpu.VMEM((nblocks * HEAD_PAD, 2 * BLK), jnp.bfloat16),
        ],
        flops=3e9,
    )(me, owners, route_slot, all_nodes, *encoded)
    held = pooled
    for mask in bits[:-3]:
        held = jnp.concatenate([held, swapped(held, mask)], axis=0)
    up, right, down = bits[-3:]
    near = {m: swapped(held, m) for m in (up, right + down, right, down)}
    over = {m: swapped(near[up], m) for m in (right + down, right, down)}
    held = [held, near[up]]
    for m in (right, down, right + down):
        held += [near[m], over[m]]
    all_pooled = jnp.concatenate(held, axis=0)
    queries, asked, member, inv = call(
        functools.partial(query_kernel, scale=log_e / math.sqrt(head_size), nodes_here=nodes_here),
        [
            shape((width, query_count)),
            shape((anchors, width), jnp.float32),
            shape((anchors, blocks)),
            shape((anchors, 1), jnp.float32),
        ],
        flops=2 * query_count * width * width,
        limit=24 * MIB,
    )(me, owners, route_slot, anchor_index, after(all_nodes, pooled), query_feat[0], w_q[0])
    anchor_kv = call(node_kernel, shape((anchors, 2 * width)), flops=1e9)(
        member, inv, asked, all_pooled, w_kv[0]
    )
    partner_kv = lax.ppermute(anchor_kv, "branch", [(0, 1), (1, 0)])
    mid = [pltpu.VMEM((width, query_count), jnp.bfloat16)]
    self_part = call(
        functools.partial(self_kernel, head_size=head_size),
        shape((query_count, width), jnp.float32),
        mid,
        flops=3e9,
    )(queries, anchor_kv, w_out[0])
    result = call(
        functools.partial(cross_kernel, head_size=head_size),
        shape((query_count, width)),
        mid,
        flops=3e9,
    )(queries, partner_kv, w_out[0], self_part)
    return result[None]


def solution(mesh):
    return jax.shard_map(
        per_device,
        mesh=mesh,
        in_specs=(
            P("branch", ("groups", "pts"), None),
            P("branch", ("groups", "pts"), None),
            P("branch", ("groups", "pts"), None),
            P("branch", "groups", None),
            P("branch", "groups"),
            P("branch", "groups"),
            P("branch", None, None),
            P("branch", None, None),
            P("branch", None, None),
            P("branch", None, None),
            P("branch", None, None),
        ),
        out_specs=P("branch", ("groups", "pts"), None),
        check_vma=False,
    )
```

```python
import math

import jax
import jax.numpy as jnp
from jax import lax
from jax.experimental import pallas as pl
from jax.experimental.pallas import tpu as pltpu
from jax.sharding import PartitionSpec as P

D = 768
HEADS = 12
BLK = 128
HEAD_PAD = 16
MIB = 1 << 20


def call(kernel, out, scratch=(), flops=0, limit=16 * MIB, far=(), far_out=False, **kw):
    whole = pl.BlockSpec(memory_space=pltpu.VMEM)
    hbm = pl.BlockSpec(memory_space=pltpu.HBM)

    def run(*args):
        specs = [
            pl.BlockSpec(memory_space=pltpu.SMEM) if a.ndim == 1 else hbm if i in far else whole
            for i, a in enumerate(args)
        ]
        whole_out = hbm if far_out else whole
        outs = [whole_out] * len(out) if isinstance(out, (list, tuple)) else whole_out
        return pl.pallas_call(
            kernel,
            out_shape=out,
            in_specs=specs,
            out_specs=outs,
            scratch_shapes=list(scratch),
            compiler_params=pltpu.CompilerParams(vmem_limit_bytes=limit),
            cost_estimate=pl.CostEstimate(flops=int(flops), bytes_accessed=0, transcendentals=0),
            **kw,
        )(*args)

    return run


def shape(dims, dtype=jnp.bfloat16):
    return jax.ShapeDtypeStruct(tuple(dims), dtype)


def matmul(a, b, dims=((1,), (0,))):
    return lax.dot_general(a, b, (dims, ((), ())), preferred_element_type=jnp.float32)


def swapped(block, mask):
    count = lax.axis_size("pts")
    return lax.ppermute(block, "pts", [(i, i ^ mask) for i in range(count)])


def masks(count):
    assert count >= 8 and count & (count - 1) == 0, count
    return [1 << b for b in reversed(range(count.bit_length() - 1))]


def after(value, *others):
    return lax.optimization_barrier((value,) + others)[0]


def placed(me, count, dims, axis, inner):
    lane = lax.broadcasted_iota(jnp.int32, dims, axis)
    place = lane // inner
    source = me
    for s, mask in enumerate(masks(count)):
        source = source ^ (((place >> s) & 1) * mask)
    return source * inner + lane % inner


def column(row):
    n = row.shape[1]
    at = lax.broadcasted_iota(jnp.int32, (n, n), 0) == lax.broadcasted_iota(jnp.int32, (n, n), 1)
    return jnp.sum(jnp.where(at, row, 0.0), axis=1, keepdims=True)


def encode_rows(rows, steps, load, w_half, w_mid_ref, hid_ref, store, ready=lambda: None):
    root = math.sqrt(2 / math.pi)

    def first(step):
        half = matmul(load(step), w_half())
        inner = half * (2 * root + 8 * 0.044715 * root * (half * half))
        hid_ref[step % 2] = (half + half * jnp.tanh(inner)).astype(jnp.bfloat16)

    first(0)
    ready()
    for step in range(steps):
        if step + 1 < steps:
            first(step + 1)
        store(step, matmul(hid_ref[step % 2], w_mid_ref[...]).astype(jnp.bfloat16))


def encode_kernel(x_ref, w_in_ref, w_mid_ref, out_ref, hid_ref, half_ref, *, base):
    rows = hid_ref.shape[1]
    half_ref[...] = w_in_ref[...] * jnp.bfloat16(0.5)

    def load(step):
        return x_ref[base + step * rows : base + (step + 1) * rows, :]

    def store(step, value):
        out_ref[step * rows : (step + 1) * rows, :] = value

    encode_rows(
        rows, out_ref.shape[0] // rows, load, lambda: half_ref[...], w_mid_ref, hid_ref, store
    )


def encode_far_kernel(
    x_far, w_in_far, w_mid_far, out_far, hid_ref, half_ref, x_ref, w_in_ref, w_mid_ref, out_ref, in_sem, out_sem, *, base
):
    rows = hid_ref.shape[1]
    steps = out_far.shape[0] // rows
    ins = [
        pltpu.make_async_copy(w_in_far, w_in_ref, in_sem.at[0]),
        pltpu.make_async_copy(x_far.at[pl.ds(base, out_far.shape[0])], x_ref, in_sem.at[1]),
        pltpu.make_async_copy(w_mid_far, w_mid_ref, in_sem.at[2]),
    ]
    for copy in ins:
        copy.start()
    ins[0].wait()
    half_ref[...] = w_in_ref[...] * jnp.bfloat16(0.5)
    ins[1].wait()
    outs = []

    def load(step):
        return x_ref[step * rows : (step + 1) * rows, :]

    def store(step, value):
        at = pl.ds(step * rows, rows)
        out_ref[at, :] = value
        outs.append(pltpu.make_async_copy(out_ref.at[at], out_far.at[at], out_sem.at[step]))
        outs[step].start()

    encode_rows(
        rows, steps, load, lambda: half_ref[...], w_mid_ref, hid_ref, store, ins[2].wait
    )
    for copy in outs:
        copy.wait()


def pool_kernel(owner_ref, slot_ref, held_ref, *refs, head_size, nodes_here):
    *enc_refs, out_ref, qm_ref, score_ref, mix_ref = refs
    me = lax.axis_index("pts").astype(jnp.int32)
    nb, width = out_ref.shape
    nodes = held_ref.shape[0]
    rows = sum(e.shape[0] for e in enc_refs) // nb
    pairs = [(e, i * 2 * rows) for e in enc_refs for i in range(e.shape[0] // (2 * rows))]
    blocks = owner_ref.shape[1]
    node_ids = (owner_ref[...] * nodes_here + slot_ref[...]).astype(jnp.float32)
    row = lax.broadcasted_iota(jnp.int32, (nb, blocks), 0) + me * nb
    col = lax.broadcasted_iota(jnp.int32, (nb, blocks), 1)
    wanted = jnp.sum(jnp.where(row == col, node_ids, 0.0), axis=1, keepdims=True)
    there = placed(me, nodes // nodes_here, (nb, nodes), 1, nodes_here).astype(jnp.float32)
    mine = (there == wanted).astype(jnp.float32).astype(jnp.bfloat16)
    asked = matmul(mine, held_ref[...]).astype(jnp.bfloat16)
    head = lax.broadcasted_iota(jnp.int32, (HEAD_PAD, width), 0)
    lane = lax.broadcasted_iota(jnp.int32, (HEAD_PAD, width), 1)
    keep = (lane // head_size == head).astype(jnp.float32)
    qm = asked[:, None, :] * keep.astype(jnp.bfloat16)[None]
    qm_ref[...] = qm.reshape(nb * HEAD_PAD, width)
    pad = 2 * HEAD_PAD
    for p, (enc_ref, at) in enumerate(pairs):
        score_ref[p * pad : (p + 1) * pad, :] = matmul(
            qm_ref[p * pad : (p + 1) * pad, :], enc_ref[at : at + 2 * rows, :], ((1,), (1,))
        )
    outs = []
    cuts = [0, len(pairs) // 2, len(pairs)]
    for begin, end in zip(cuts[:-1], cuts[1:]):
        at = slice(begin * pad, end * pad)
        shape3 = (end - begin, pad, 2 * rows)
        scores = score_ref[at, :].reshape(shape3) * (1.0 / math.sqrt(head_size))
        own = lax.broadcasted_iota(jnp.int32, shape3, 1) // HEAD_PAD == lax.broadcasted_iota(
            jnp.int32, shape3, 2
        ) // rows
        top = jnp.max(jnp.where(own, scores, -jnp.inf), axis=2, keepdims=True)
        part = jnp.where(own, jnp.exp(scores - top), 0.0)
        part = part * (1.0 / jnp.sum(part, axis=2, keepdims=True))
        mix_ref[at, :] = part.astype(jnp.bfloat16).reshape((end - begin) * pad, 2 * rows)
        for p in range(begin, end):
            enc_ref, row = pairs[p]
            mixed = matmul(mix_ref[p * pad : (p + 1) * pad, :], enc_ref[row : row + 2 * rows, :])
            outs.append(jnp.sum(mixed.reshape(2, HEAD_PAD, width) * keep[None], axis=1))
    out_ref[...] = jnp.concatenate(outs, axis=0).astype(jnp.bfloat16)


def query_kernel(
    owner_ref,
    slot_ref,
    anchor_ref,
    held_ref,
    feat_ref,
    w_ref,
    out_ref,
    asked_ref,
    member_ref,
    inv_ref,
    *,
    scale,
    nodes_here,
):
    me = lax.axis_index("pts").astype(jnp.int32)
    blocks = owner_ref.shape[1]
    nodes = held_ref.shape[0]
    anchors = anchor_ref.shape[1]
    count = nodes // nodes_here
    queries = matmul(feat_ref[...], w_ref[...]) * scale
    out_ref[...] = queries.astype(jnp.bfloat16).T
    node_ids = (owner_ref[...] * nodes_here + slot_ref[...]).astype(jnp.float32)
    wanted = column(anchor_ref[...].astype(jnp.float32))
    member = (node_ids == wanted).astype(jnp.float32)
    inv_ref[...] = 1.0 / jnp.maximum(jnp.sum(member, axis=1, keepdims=True), 1.0)
    row = lax.broadcasted_iota(jnp.int32, (blocks, blocks), 0)
    moved = row == placed(me, count, (blocks, blocks), 1, blocks // count)
    moved = moved.astype(jnp.float32).astype(jnp.bfloat16)
    member_ref[...] = matmul(member.astype(jnp.bfloat16), moved).astype(jnp.bfloat16)
    there = placed(me, count, (anchors, nodes), 1, nodes_here).astype(jnp.float32)
    pick = (there == wanted).astype(jnp.float32).astype(jnp.bfloat16)
    asked_ref[...] = matmul(pick, held_ref[...])


def node_kernel(member_ref, inv_ref, asked_ref, pooled_ref, w_kv_ref, kv_ref):
    value = asked_ref[...] + matmul(member_ref[...], pooled_ref[...]) * inv_ref[...]
    mean = jnp.mean(value * value, axis=1, keepdims=True)
    feat = (value * lax.rsqrt(mean + 1e-06)).astype(jnp.bfloat16)
    kv_ref[...] = matmul(feat, w_kv_ref[...]).astype(jnp.bfloat16)


def attend(q_ref, kv_ref, out_ref, head_size):
    width, _ = q_ref.shape
    anchors = kv_ref.shape[0]
    pair = 2 * head_size
    lane = lax.broadcasted_iota(jnp.int32, (anchors, pair), 1)

    def score(j):
        at = slice(j * pair, (j + 1) * pair)
        keys = kv_ref[:, at]
        zero = jnp.zeros_like(keys)
        both = jnp.concatenate(
            [jnp.where(lane < head_size, keys, zero), jnp.where(lane >= head_size, keys, zero)], axis=0
        )
        return matmul(both, q_ref[at, :])

    def weigh(j, scores):
        values = kv_ref[:, width + j * pair : width + (j + 1) * pair].T
        ones = jnp.ones((HEAD_PAD, anchors), jnp.bfloat16)
        for h in range(2):
            part = scores[h * anchors : (h + 1) * anchors]
            part = jnp.exp2(part - jnp.max(part, axis=0, keepdims=True)).astype(jnp.bfloat16)
            left = jnp.concatenate([values[h * head_size : (h + 1) * head_size], ones], axis=0)
            got = matmul(left, part)
            got = got[:head_size] * (1.0 / got[head_size : head_size + 1])
            base = j * pair + h * head_size
            out_ref[base : base + head_size, :] = got.astype(jnp.bfloat16)

    ahead = score(0)
    for j in range(width // pair):
        scores = ahead
        if j + 1 < width // pair:
            ahead = score(j + 1)
        weigh(j, scores)


def self_kernel(q_ref, kv_ref, w_ref, out_ref, mid_ref, *, head_size):
    attend(q_ref, kv_ref, mid_ref, head_size)
    width = mid_ref.shape[0]
    out_ref[...] = matmul(mid_ref[...].T, w_ref[:width, :])


def cross_kernel(q_ref, kv_ref, w_ref, own_ref, out_ref, mid_ref, *, head_size):
    attend(q_ref, kv_ref, mid_ref, head_size)
    width = mid_ref.shape[0]
    out_ref[...] = (own_ref[...] + matmul(mid_ref[...].T, w_ref[width:, :])).astype(jnp.bfloat16)


def per_device(
    point_feat,
    query_feat,
    supernode_query,
    route_owner,
    route_slot,
    anchor_index,
    w_in,
    w_mid,
    w_q,
    w_kv,
    w_out,
):
    import functools

    head_size = D // HEADS
    shard_count = lax.axis_size("pts")
    points = point_feat[0]
    nblocks = points.shape[0] // BLK
    own = supernode_query[0]
    nodes_here, width = own.shape
    owners = route_owner.reshape(1, -1)
    blocks = owners.shape[1]
    nodes = nodes_here * shard_count
    anchors = anchor_index.shape[1]
    query_count = query_feat.shape[1]

    bits = masks(shard_count)
    rows = 2 * BLK
    log_e = 1.0 / math.log(2.0)

    def encode(points, begin, end, near):
        scratch = [
            pltpu.VMEM((2, rows, width), jnp.bfloat16),
            pltpu.VMEM(w_in.shape[1:], jnp.bfloat16),
        ]
        if not near:
            scratch += [
                pltpu.VMEM((end - begin, points.shape[1]), jnp.bfloat16),
                pltpu.VMEM(w_in.shape[1:], jnp.bfloat16),
                pltpu.VMEM(w_mid.shape[1:], jnp.bfloat16),
                pltpu.VMEM((end - begin, width), jnp.bfloat16),
                pltpu.SemaphoreType.DMA((3,)),
                pltpu.SemaphoreType.DMA(((end - begin) // rows,)),
            ]
        return call(
            functools.partial(encode_kernel if near else encode_far_kernel, base=begin),
            shape((end - begin, width)),
            scratch,
            flops=2 * (end - begin) * width * (width + points.shape[1]),
            far=() if near else (0, 1, 2),
            far_out=not near,
            limit=16 * MIB if near else 60 * MIB,
        )(points, w_in[0], w_mid[0])

    def pieces(stages):
        pairs = nblocks // 2
        cuts = [rows * (pairs * s // stages) for s in range(stages + 1)]
        cuts[1] -= rows
        return list(zip(cuts[:-1], cuts[1:]))

    stages = bits[:-2] + [bits[-2:]]
    held, encoded = own, []
    for stage, (begin, end) in zip(stages, pieces(len(stages))):
        last = isinstance(stage, list)
        got = [swapped(held, m) for m in (stage + [sum(stage)] if last else [stage])]
        encoded.append(encode(after(points, held) if encoded else points, begin, end, last))
        got = [after(g, encoded[-1]) for g in got]
        held = jnp.concatenate([held] + got, axis=0)
    all_nodes = held
    pooled = call(
        functools.partial(pool_kernel, head_size=head_size, nodes_here=nodes_here),
        shape((nblocks, width)),
        [
            pltpu.VMEM((nblocks * HEAD_PAD, width), jnp.bfloat16),
            pltpu.VMEM((nblocks * HEAD_PAD, 2 * BLK), jnp.float32),
            pltpu.VMEM((nblocks * HEAD_PAD, 2 * BLK), jnp.bfloat16),
        ],
        flops=3e9,
    )(owners, route_slot, all_nodes, *encoded)
    held = pooled
    for mask in bits[:-3]:
        held = jnp.concatenate([held, swapped(held, mask)], axis=0)
    up, right, down = bits[-3:]
    near = {m: swapped(held, m) for m in (up, right + down, right, down)}
    over = {m: swapped(near[up], m) for m in (right + down, right, down)}
    held = [held, near[up]]
    for m in (right, down, right + down):
        held += [near[m], over[m]]
    all_pooled = jnp.concatenate(held, axis=0)
    queries, asked, member, inv = call(
        functools.partial(query_kernel, scale=log_e / math.sqrt(head_size), nodes_here=nodes_here),
        [
            shape((width, query_count)),
            shape((anchors, width), jnp.float32),
            shape((anchors, blocks)),
            shape((anchors, 1), jnp.float32),
        ],
        flops=2 * query_count * width * width,
        limit=24 * MIB,
    )(owners, route_slot, anchor_index, after(all_nodes, pooled), query_feat[0], w_q[0])
    anchor_kv = call(node_kernel, shape((anchors, 2 * width)), flops=1e9)(
        member, inv, asked, all_pooled, w_kv[0]
    )
    partner_kv = lax.ppermute(anchor_kv, "branch", [(0, 1), (1, 0)])
    mid = [pltpu.VMEM((width, query_count), jnp.bfloat16)]
    self_part = call(
        functools.partial(self_kernel, head_size=head_size),
        shape((query_count, width), jnp.float32),
        mid,
        flops=3e9,
    )(queries, anchor_kv, w_out[0])
    result = call(
        functools.partial(cross_kernel, head_size=head_size),
        shape((query_count, width)),
        mid,
        flops=3e9,
    )(queries, partner_kv, w_out[0], self_part)
    return result[None]


def solution(mesh):
    return jax.shard_map(
        per_device,
        mesh=mesh,
        in_specs=(
            P("branch", ("groups", "pts"), None),
            P("branch", ("groups", "pts"), None),
            P("branch", ("groups", "pts"), None),
            P("branch", "groups", None),
            P("branch", "groups"),
            P("branch", "groups"),
            P("branch", None, None),
            P("branch", None, None),
            P("branch", None, None),
            P("branch", None, None),
            P("branch", None, None),
        ),
        out_specs=P("branch", ("groups", "pts"), None),
        check_vma=False,
    )
```

```python
import math

import jax
import jax.numpy as jnp
from jax import lax
from jax.experimental import pallas as pl
from jax.experimental.pallas import tpu as pltpu
from jax.sharding import PartitionSpec as P

D = 768
HEADS = 12
BLK = 128
HEAD_PAD = 16
MIB = 1 << 20


def call(kernel, out, scratch=(), flops=0, limit=16 * MIB, far=(), far_out=False, **kw):
    whole = pl.BlockSpec(memory_space=pltpu.VMEM)
    hbm = pl.BlockSpec(memory_space=pltpu.HBM)

    def run(*args):
        specs = [
            pl.BlockSpec(memory_space=pltpu.SMEM) if a.ndim == 1 else hbm if i in far else whole
            for i, a in enumerate(args)
        ]
        whole_out = hbm if far_out else whole
        outs = [whole_out] * len(out) if isinstance(out, (list, tuple)) else whole_out
        return pl.pallas_call(
            kernel,
            out_shape=out,
            in_specs=specs,
            out_specs=outs,
            scratch_shapes=list(scratch),
            compiler_params=pltpu.CompilerParams(vmem_limit_bytes=limit),
            cost_estimate=pl.CostEstimate(flops=int(flops), bytes_accessed=0, transcendentals=0),
            **kw,
        )(*args)

    return run


def shape(dims, dtype=jnp.bfloat16):
    return jax.ShapeDtypeStruct(tuple(dims), dtype)


def matmul(a, b, dims=((1,), (0,))):
    return lax.dot_general(a, b, (dims, ((), ())), preferred_element_type=jnp.float32)


def swapped(block, mask):
    count = lax.axis_size("pts")
    return lax.ppermute(block, "pts", [(i, i ^ mask) for i in range(count)])


def masks(count):
    assert count >= 8 and count & (count - 1) == 0, count
    return [1 << b for b in reversed(range(count.bit_length() - 1))]


def after(value, *others):
    return lax.optimization_barrier((value,) + others)[0]


def placed(me, count, dims, axis, inner):
    lane = lax.broadcasted_iota(jnp.int32, dims, axis)
    place = lane // inner
    source = me
    for s, mask in enumerate(masks(count)):
        source = source ^ (((place >> s) & 1) * mask)
    return source * inner + lane % inner


def column(row):
    n = row.shape[1]
    at = lax.broadcasted_iota(jnp.int32, (n, n), 0) == lax.broadcasted_iota(jnp.int32, (n, n), 1)
    return jnp.sum(jnp.where(at, row, 0.0), axis=1, keepdims=True)


def encode_rows(rows, steps, load, w_half, w_mid_ref, hid_ref, store, ready=lambda: None):
    root = math.sqrt(2 / math.pi)

    def first(step):
        half = matmul(load(step), w_half())
        inner = half * (2 * root + 8 * 0.044715 * root * (half * half))
        hid_ref[step % 2] = (half + half * jnp.tanh(inner)).astype(jnp.bfloat16)

    first(0)
    ready()
    for step in range(steps):
        if step + 1 < steps:
            first(step + 1)
        store(step, matmul(hid_ref[step % 2], w_mid_ref[...]).astype(jnp.bfloat16))


def encode_kernel(
    x_ref, w_in_ref, w_mid_ref, owner_ref, slot_ref, out_ref, mine_ref, hid_ref, half_ref, *, base, nodes_here
):
    rows = hid_ref.shape[1]
    half_ref[...] = w_in_ref[...] * jnp.bfloat16(0.5)
    me = lax.axis_index("pts").astype(jnp.int32)
    nb, nodes = mine_ref.shape
    blocks = owner_ref.shape[1]
    node_ids = (owner_ref[...] * nodes_here + slot_ref[...]).astype(jnp.float32)
    row = lax.broadcasted_iota(jnp.int32, (nb, blocks), 0) + me * nb
    col = lax.broadcasted_iota(jnp.int32, (nb, blocks), 1)
    wanted = jnp.sum(jnp.where(row == col, node_ids, 0.0), axis=1, keepdims=True)
    there = placed(me, nodes // nodes_here, (nb, nodes), 1, nodes_here).astype(jnp.float32)
    mine_ref[...] = (there == wanted).astype(jnp.float32).astype(jnp.bfloat16)

    def load(step):
        return x_ref[base + step * rows : base + (step + 1) * rows, :]

    def store(step, value):
        out_ref[step * rows : (step + 1) * rows, :] = value

    encode_rows(
        rows, out_ref.shape[0] // rows, load, lambda: half_ref[...], w_mid_ref, hid_ref, store
    )


def encode_far_kernel(
    x_far, w_in_far, w_mid_far, out_far, hid_ref, half_ref, x_ref, w_in_ref, w_mid_ref, out_ref, in_sem, out_sem, *, base
):
    rows = hid_ref.shape[1]
    steps = out_far.shape[0] // rows
    ins = [
        pltpu.make_async_copy(w_in_far, w_in_ref, in_sem.at[0]),
        pltpu.make_async_copy(x_far.at[pl.ds(base, rows)], x_ref.at[pl.ds(0, rows)], in_sem.at[1]),
        pltpu.make_async_copy(w_mid_far, w_mid_ref, in_sem.at[2]),
        pltpu.make_async_copy(
            x_far.at[pl.ds(base + rows, out_far.shape[0] - rows)],
            x_ref.at[pl.ds(rows, out_far.shape[0] - rows)],
            in_sem.at[3],
        ),
    ]
    for copy in ins:
        copy.start()
    ins[0].wait()
    half_ref[...] = w_in_ref[...] * jnp.bfloat16(0.5)
    ins[1].wait()
    outs = []

    def ready():
        ins[2].wait()
        ins[3].wait()

    def load(step):
        return x_ref[step * rows : (step + 1) * rows, :]

    def store(step, value):
        at = pl.ds(step * rows, rows)
        out_ref[at, :] = value
        outs.append(pltpu.make_async_copy(out_ref.at[at], out_far.at[at], out_sem.at[step]))
        outs[step].start()

    encode_rows(
        rows, steps, load, lambda: half_ref[...], w_mid_ref, hid_ref, store, ready
    )
    for copy in outs:
        copy.wait()


def pool_kernel(mine_ref, held_ref, *refs, head_size):
    *enc_refs, out_ref, qm_ref, score_ref, mix_ref = refs
    nb, width = out_ref.shape
    rows = sum(e.shape[0] for e in enc_refs) // nb
    pairs = [(e, i * 2 * rows) for e in enc_refs for i in range(e.shape[0] // (2 * rows))]
    asked = matmul(mine_ref[...], held_ref[...]).astype(jnp.bfloat16)
    head = lax.broadcasted_iota(jnp.int32, (HEAD_PAD, width), 0)
    lane = lax.broadcasted_iota(jnp.int32, (HEAD_PAD, width), 1)
    keep = (lane // head_size == head).astype(jnp.float32)
    row = lax.broadcasted_iota(jnp.int32, (nb * HEAD_PAD, nb), 0) // HEAD_PAD
    col = lax.broadcasted_iota(jnp.int32, (nb * HEAD_PAD, nb), 1)
    each = matmul((row == col).astype(jnp.float32).astype(jnp.bfloat16), asked)
    qm = each.reshape(nb, HEAD_PAD, width) * keep[None]
    qm_ref[...] = qm.astype(jnp.bfloat16).reshape(nb * HEAD_PAD, width)
    pad = 2 * HEAD_PAD
    for p, (enc_ref, at) in enumerate(pairs):
        score_ref[p * pad : (p + 1) * pad, :] = matmul(
            qm_ref[p * pad : (p + 1) * pad, :], enc_ref[at : at + 2 * rows, :], ((1,), (1,))
        )
    outs = []
    cuts = [0, len(pairs) // 2, len(pairs)]
    for begin, end in zip(cuts[:-1], cuts[1:]):
        at = slice(begin * pad, end * pad)
        shape3 = (end - begin, pad, 2 * rows)
        own = lax.broadcasted_iota(jnp.int32, shape3, 1) // HEAD_PAD == lax.broadcasted_iota(
            jnp.int32, shape3, 2
        ) // rows
        scale = 1.0 / (math.sqrt(head_size) * math.log(2.0))
        scores = jnp.where(own, score_ref[at, :].reshape(shape3) * scale, -jnp.inf)
        part = jnp.exp2(scores - jnp.max(scores, axis=2, keepdims=True))
        part = part * (1.0 / jnp.sum(part, axis=2, keepdims=True))
        mix_ref[at, :] = part.astype(jnp.bfloat16).reshape((end - begin) * pad, 2 * rows)
        for p in range(begin, end):
            enc_ref, row = pairs[p]
            mixed = matmul(mix_ref[p * pad : (p + 1) * pad, :], enc_ref[row : row + 2 * rows, :])
            outs.append(jnp.sum(mixed.reshape(2, HEAD_PAD, width) * keep[None], axis=1))
    out_ref[...] = jnp.concatenate(outs, axis=0).astype(jnp.bfloat16)


def query_kernel(
    owner_ref,
    slot_ref,
    anchor_ref,
    held_ref,
    feat_ref,
    w_ref,
    out_ref,
    asked_ref,
    member_ref,
    inv_ref,
    *,
    scale,
    nodes_here,
):
    me = lax.axis_index("pts").astype(jnp.int32)
    blocks = owner_ref.shape[1]
    nodes = held_ref.shape[0]
    anchors = anchor_ref.shape[1]
    count = nodes // nodes_here
    queries = matmul(feat_ref[...], w_ref[...]) * scale
    out_ref[...] = queries.astype(jnp.bfloat16).T
    node_ids = (owner_ref[...] * nodes_here + slot_ref[...]).astype(jnp.float32)
    wanted = column(anchor_ref[...].astype(jnp.float32))
    member = (node_ids == wanted).astype(jnp.float32)
    inv_ref[...] = 1.0 / jnp.maximum(jnp.sum(member, axis=1, keepdims=True), 1.0)
    row = lax.broadcasted_iota(jnp.int32, (blocks, blocks), 0)
    moved = row == placed(me, count, (blocks, blocks), 1, blocks // count)
    moved = moved.astype(jnp.float32).astype(jnp.bfloat16)
    member_ref[...] = matmul(member.astype(jnp.bfloat16), moved).astype(jnp.bfloat16)
    there = placed(me, count, (anchors, nodes), 1, nodes_here).astype(jnp.float32)
    pick = (there == wanted).astype(jnp.float32).astype(jnp.bfloat16)
    asked_ref[...] = matmul(pick, held_ref[...])


def node_kernel(member_ref, inv_ref, asked_ref, pooled_ref, w_kv_ref, kv_ref):
    value = asked_ref[...] + matmul(member_ref[...], pooled_ref[...]) * inv_ref[...]
    mean = jnp.mean(value * value, axis=1, keepdims=True)
    feat = (value * lax.rsqrt(mean + 1e-06)).astype(jnp.bfloat16)
    kv_ref[...] = matmul(feat, w_kv_ref[...]).astype(jnp.bfloat16)


def attend(q_ref, kv_ref, out_ref, head_size):
    width, _ = q_ref.shape
    anchors = kv_ref.shape[0]
    pair = 2 * head_size
    lane = lax.broadcasted_iota(jnp.int32, (anchors, pair), 1)

    def score(j):
        at = slice(j * pair, (j + 1) * pair)
        keys = kv_ref[:, at]
        zero = jnp.zeros_like(keys)
        both = jnp.concatenate(
            [jnp.where(lane < head_size, keys, zero), jnp.where(lane >= head_size, keys, zero)], axis=0
        )
        return matmul(both, q_ref[at, :])

    def weigh(j, scores):
        values = kv_ref[:, width + j * pair : width + (j + 1) * pair].T
        ones = jnp.ones((HEAD_PAD, anchors), jnp.bfloat16)
        for h in range(2):
            part = scores[h * anchors : (h + 1) * anchors]
            part = jnp.exp2(part - jnp.max(part, axis=0, keepdims=True)).astype(jnp.bfloat16)
            left = jnp.concatenate([values[h * head_size : (h + 1) * head_size], ones], axis=0)
            got = matmul(left, part)
            got = got[:head_size] * (1.0 / got[head_size : head_size + 1])
            base = j * pair + h * head_size
            out_ref[base : base + head_size, :] = got.astype(jnp.bfloat16)

    ahead = score(0)
    for j in range(width // pair):
        scores = ahead
        if j + 1 < width // pair:
            ahead = score(j + 1)
        weigh(j, scores)


def self_kernel(q_ref, kv_ref, w_ref, out_ref, mid_ref, *, head_size):
    attend(q_ref, kv_ref, mid_ref, head_size)
    width = mid_ref.shape[0]
    out_ref[...] = matmul(mid_ref[...].T, w_ref[:width, :])


def cross_kernel(q_ref, kv_ref, w_ref, own_ref, out_ref, mid_ref, *, head_size):
    attend(q_ref, kv_ref, mid_ref, head_size)
    width = mid_ref.shape[0]
    out_ref[...] = (own_ref[...] + matmul(mid_ref[...].T, w_ref[width:, :])).astype(jnp.bfloat16)


def per_device(
    point_feat,
    query_feat,
    supernode_query,
    route_owner,
    route_slot,
    anchor_index,
    w_in,
    w_mid,
    w_q,
    w_kv,
    w_out,
):
    import functools

    head_size = D // HEADS
    shard_count = lax.axis_size("pts")
    points = point_feat[0]
    nblocks = points.shape[0] // BLK
    own = supernode_query[0]
    nodes_here, width = own.shape
    owners = route_owner.reshape(1, -1)
    blocks = owners.shape[1]
    nodes = nodes_here * shard_count
    anchors = anchor_index.shape[1]
    query_count = query_feat.shape[1]

    bits = masks(shard_count)
    rows = 2 * BLK
    log_e = 1.0 / math.log(2.0)

    def encode(points, begin, end, near):
        scratch = [
            pltpu.VMEM((2, rows, width), jnp.bfloat16),
            pltpu.VMEM(w_in.shape[1:], jnp.bfloat16),
        ]
        if not near:
            scratch += [
                pltpu.VMEM((end - begin, points.shape[1]), jnp.bfloat16),
                pltpu.VMEM(w_in.shape[1:], jnp.bfloat16),
                pltpu.VMEM(w_mid.shape[1:], jnp.bfloat16),
                pltpu.VMEM((end - begin, width), jnp.bfloat16),
                pltpu.SemaphoreType.DMA((4,)),
                pltpu.SemaphoreType.DMA(((end - begin) // rows,)),
            ]
        if near:
            return call(
                functools.partial(encode_kernel, base=begin, nodes_here=nodes_here),
                [shape((end - begin, width)), shape((nblocks, nodes))],
                scratch,
                flops=2 * (end - begin) * width * (width + points.shape[1]),
            )(points, w_in[0], w_mid[0], owners, route_slot)
        return call(
            functools.partial(encode_far_kernel, base=begin),
            shape((end - begin, width)),
            scratch,
            flops=2 * (end - begin) * width * (width + points.shape[1]),
            far=(0, 1, 2),
            far_out=True,
            limit=60 * MIB,
        )(points, w_in[0], w_mid[0])

    def pieces(stages):
        pairs = nblocks // 2
        cuts = [rows * (pairs * s // stages) for s in range(stages + 1)]
        cuts[1] -= rows
        return list(zip(cuts[:-1], cuts[1:]))

    stages = bits[:-2] + [bits[-2:]]
    held, encoded = own, []
    for stage, (begin, end) in zip(stages, pieces(len(stages))):
        last = isinstance(stage, list)
        got = [swapped(held, m) for m in (stage + [sum(stage)] if last else [stage])]
        done = encode(after(points, held) if encoded else points, begin, end, last)
        if last:
            done, mine = done
        encoded.append(done)
        got = [after(g, encoded[-1]) for g in got]
        held = jnp.concatenate([held] + got, axis=0)
    all_nodes = held
    pooled = call(
        functools.partial(pool_kernel, head_size=head_size),
        shape((nblocks, width)),
        [
            pltpu.VMEM((nblocks * HEAD_PAD, width), jnp.bfloat16),
            pltpu.VMEM((nblocks * HEAD_PAD, 2 * BLK), jnp.float32),
            pltpu.VMEM((nblocks * HEAD_PAD, 2 * BLK), jnp.bfloat16),
        ],
        flops=3e9,
    )(mine, all_nodes, *encoded)
    held = pooled
    for mask in bits[:-3]:
        held = jnp.concatenate([held, swapped(held, mask)], axis=0)
    up, right, down = bits[-3:]
    near = {m: swapped(held, m) for m in (up, right + down, right, down)}
    over = {m: swapped(near[up], m) for m in (right + down, right, down)}
    held = [held, near[up]]
    for m in (right, down, right + down):
        held += [near[m], over[m]]
    all_pooled = jnp.concatenate(held, axis=0)
    queries, asked, member, inv = call(
        functools.partial(query_kernel, scale=log_e / math.sqrt(head_size), nodes_here=nodes_here),
        [
            shape((width, query_count)),
            shape((anchors, width), jnp.float32),
            shape((anchors, blocks)),
            shape((anchors, 1), jnp.float32),
        ],
        flops=2 * query_count * width * width,
        limit=24 * MIB,
    )(owners, route_slot, anchor_index, after(all_nodes, pooled), query_feat[0], w_q[0])
    anchor_kv = call(node_kernel, shape((anchors, 2 * width)), flops=1e9)(
        member, inv, asked, all_pooled, w_kv[0]
    )
    partner_kv = lax.ppermute(anchor_kv, "branch", [(0, 1), (1, 0)])
    mid = [pltpu.VMEM((width, query_count), jnp.bfloat16)]
    self_part = call(
        functools.partial(self_kernel, head_size=head_size),
        shape((query_count, width), jnp.float32),
        mid,
        flops=3e9,
    )(queries, anchor_kv, w_out[0])
    result = call(
        functools.partial(cross_kernel, head_size=head_size),
        shape((query_count, width)),
        mid,
        flops=3e9,
    )(queries, partner_kv, w_out[0], self_part)
    return result[None]


def solution(mesh):
    return jax.shard_map(
        per_device,
        mesh=mesh,
        in_specs=(
            P("branch", ("groups", "pts"), None),
            P("branch", ("groups", "pts"), None),
            P("branch", ("groups", "pts"), None),
            P("branch", "groups", None),
            P("branch", "groups"),
            P("branch", "groups"),
            P("branch", None, None),
            P("branch", None, None),
            P("branch", None, None),
            P("branch", None, None),
            P("branch", None, None),
        ),
        out_specs=P("branch", ("groups", "pts"), None),
        check_vma=False,
    )
```

```python
import math

import jax
import jax.numpy as jnp
from jax import lax
from jax.experimental import pallas as pl
from jax.experimental.pallas import tpu as pltpu
from jax.sharding import PartitionSpec as P

D = 768
HEADS = 12
BLK = 128
HEAD_PAD = 16
MIB = 1 << 20


def call(kernel, out, scratch=(), flops=0, limit=16 * MIB, far=(), far_out=False, **kw):
    whole = pl.BlockSpec(memory_space=pltpu.VMEM)
    hbm = pl.BlockSpec(memory_space=pltpu.HBM)

    def run(*args):
        specs = [
            pl.BlockSpec(memory_space=pltpu.SMEM) if a.ndim == 1 else hbm if i in far else whole
            for i, a in enumerate(args)
        ]
        whole_out = hbm if far_out else whole
        outs = [whole_out] * len(out) if isinstance(out, (list, tuple)) else whole_out
        return pl.pallas_call(
            kernel,
            out_shape=out,
            in_specs=specs,
            out_specs=outs,
            scratch_shapes=list(scratch),
            compiler_params=pltpu.CompilerParams(vmem_limit_bytes=limit),
            cost_estimate=pl.CostEstimate(flops=int(flops), bytes_accessed=0, transcendentals=0),
            **kw,
        )(*args)

    return run


def shape(dims, dtype=jnp.bfloat16):
    return jax.ShapeDtypeStruct(tuple(dims), dtype)


def matmul(a, b, dims=((1,), (0,))):
    return lax.dot_general(a, b, (dims, ((), ())), preferred_element_type=jnp.float32)


def swapped(block, mask):
    count = lax.axis_size("pts")
    return lax.ppermute(block, "pts", [(i, i ^ mask) for i in range(count)])


def masks(count):
    assert count >= 8 and count & (count - 1) == 0, count
    return [1 << b for b in reversed(range(count.bit_length() - 1))]


def after(value, *others):
    return lax.optimization_barrier((value,) + others)[0]


def placed(me, count, dims, axis, inner):
    lane = lax.broadcasted_iota(jnp.int32, dims, axis)
    place = lane // inner
    source = me
    for s, mask in enumerate(masks(count)):
        source = source ^ (((place >> s) & 1) * mask)
    return source * inner + lane % inner


def column(row):
    n = row.shape[1]
    at = lax.broadcasted_iota(jnp.int32, (n, n), 0) == lax.broadcasted_iota(jnp.int32, (n, n), 1)
    return jnp.sum(jnp.where(at, row, 0.0), axis=1, keepdims=True)


def encode_rows(rows, steps, load, w_half, w_mid_ref, hid_ref, store, ready=lambda: None):
    root = math.sqrt(2 / math.pi)

    def first(step):
        half = matmul(load(step), w_half())
        inner = half * (2 * root + 8 * 0.044715 * root * (half * half))
        hid_ref[step % 2] = (half + half * jnp.tanh(inner)).astype(jnp.bfloat16)

    first(0)
    ready()
    for step in range(steps):
        if step + 1 < steps:
            first(step + 1)
        store(step, matmul(hid_ref[step % 2], w_mid_ref[...]).astype(jnp.bfloat16))


def encode_kernel(
    x_ref, w_in_ref, w_mid_ref, owner_ref, slot_ref, out_ref, mine_ref, hid_ref, half_ref, *, base, nodes_here
):
    rows = hid_ref.shape[1]
    half_ref[...] = w_in_ref[...] * jnp.bfloat16(0.5)
    me = lax.axis_index("pts").astype(jnp.int32)
    nb, nodes = mine_ref.shape
    blocks = owner_ref.shape[1]
    node_ids = (owner_ref[...] * nodes_here + slot_ref[...]).astype(jnp.float32)
    row = lax.broadcasted_iota(jnp.int32, (nb, blocks), 0) + me * nb
    col = lax.broadcasted_iota(jnp.int32, (nb, blocks), 1)
    wanted = jnp.sum(jnp.where(row == col, node_ids, 0.0), axis=1, keepdims=True)
    there = placed(me, nodes // nodes_here, (nb, nodes), 1, nodes_here).astype(jnp.float32)
    mine_ref[...] = (there == wanted).astype(jnp.float32).astype(jnp.bfloat16)

    def load(step):
        return x_ref[base + step * rows : base + (step + 1) * rows, :]

    def store(step, value):
        out_ref[step * rows : (step + 1) * rows, :] = value

    encode_rows(
        rows, out_ref.shape[0] // rows, load, lambda: half_ref[...], w_mid_ref, hid_ref, store
    )


def encode_far_kernel(
    x_far, w_in_far, w_mid_far, out_far, hid_ref, half_ref, x_ref, w_in_ref, w_mid_ref, out_ref, in_sem, out_sem, *, base
):
    rows = hid_ref.shape[1]
    steps = out_far.shape[0] // rows
    ins = [
        pltpu.make_async_copy(w_in_far, w_in_ref, in_sem.at[0]),
        pltpu.make_async_copy(x_far.at[pl.ds(base, rows)], x_ref.at[pl.ds(0, rows)], in_sem.at[1]),
        pltpu.make_async_copy(w_mid_far, w_mid_ref, in_sem.at[2]),
        pltpu.make_async_copy(
            x_far.at[pl.ds(base + rows, out_far.shape[0] - rows)],
            x_ref.at[pl.ds(rows, out_far.shape[0] - rows)],
            in_sem.at[3],
        ),
    ]
    for copy in ins:
        copy.start()
    ins[0].wait()
    half_ref[...] = w_in_ref[...] * jnp.bfloat16(0.5)
    ins[1].wait()
    outs = []

    def ready():
        ins[2].wait()
        ins[3].wait()

    def load(step):
        return x_ref[step * rows : (step + 1) * rows, :]

    def store(step, value):
        at = pl.ds(step * rows, rows)
        out_ref[at, :] = value
        outs.append(pltpu.make_async_copy(out_ref.at[at], out_far.at[at], out_sem.at[step]))
        outs[step].start()

    encode_rows(
        rows, steps, load, lambda: half_ref[...], w_mid_ref, hid_ref, store, ready
    )
    for copy in outs:
        copy.wait()


def pool_kernel(mine_ref, held_ref, *refs, head_size):
    *enc_refs, out_ref, qm_ref, score_ref, mix_ref = refs
    nb, width = out_ref.shape
    rows = sum(e.shape[0] for e in enc_refs) // nb
    pairs = [(e, i * 2 * rows) for e in enc_refs for i in range(e.shape[0] // (2 * rows))]
    asked = matmul(mine_ref[...], held_ref[...]).astype(jnp.bfloat16)
    head = lax.broadcasted_iota(jnp.int32, (HEAD_PAD, width), 0)
    lane = lax.broadcasted_iota(jnp.int32, (HEAD_PAD, width), 1)
    keep = (lane // head_size == head).astype(jnp.float32)
    row = lax.broadcasted_iota(jnp.int32, (nb * HEAD_PAD, nb), 0) // HEAD_PAD
    col = lax.broadcasted_iota(jnp.int32, (nb * HEAD_PAD, nb), 1)
    each = matmul((row == col).astype(jnp.float32).astype(jnp.bfloat16), asked)
    qm = each.reshape(nb, HEAD_PAD, width) * keep[None]
    qm_ref[...] = qm.astype(jnp.bfloat16).reshape(nb * HEAD_PAD, width)
    pad = 2 * HEAD_PAD
    for p, (enc_ref, at) in enumerate(pairs):
        score_ref[p * pad : (p + 1) * pad, :] = matmul(
            qm_ref[p * pad : (p + 1) * pad, :], enc_ref[at : at + 2 * rows, :], ((1,), (1,))
        )
    outs = []
    cuts = [0, len(pairs) // 2, len(pairs)]
    for begin, end in zip(cuts[:-1], cuts[1:]):
        at = slice(begin * pad, end * pad)
        shape3 = (end - begin, pad, 2 * rows)
        own = lax.broadcasted_iota(jnp.int32, shape3, 1) // HEAD_PAD == lax.broadcasted_iota(
            jnp.int32, shape3, 2
        ) // rows
        scale = 1.0 / (math.sqrt(head_size) * math.log(2.0))
        scores = jnp.where(own, score_ref[at, :].reshape(shape3) * scale, -jnp.inf)
        part = jnp.exp2(scores - jnp.max(scores, axis=2, keepdims=True))
        part = part * (1.0 / jnp.sum(part, axis=2, keepdims=True))
        mix_ref[at, :] = part.astype(jnp.bfloat16).reshape((end - begin) * pad, 2 * rows)
        for p in range(begin, end):
            enc_ref, row = pairs[p]
            mixed = matmul(mix_ref[p * pad : (p + 1) * pad, :], enc_ref[row : row + 2 * rows, :])
            outs.append(jnp.sum(mixed.reshape(2, HEAD_PAD, width) * keep[None], axis=1))
    out_ref[...] = jnp.concatenate(outs, axis=0).astype(jnp.bfloat16)


def query_kernel(
    owner_ref,
    slot_ref,
    anchor_ref,
    held_ref,
    feat_ref,
    w_ref,
    out_ref,
    asked_ref,
    member_ref,
    inv_ref,
    *,
    scale,
    nodes_here,
):
    me = lax.axis_index("pts").astype(jnp.int32)
    blocks = owner_ref.shape[1]
    nodes = held_ref.shape[0]
    anchors = anchor_ref.shape[1]
    count = nodes // nodes_here
    queries = matmul(feat_ref[...], w_ref[...]) * scale
    out_ref[...] = queries.astype(jnp.bfloat16).T
    node_ids = (owner_ref[...] * nodes_here + slot_ref[...]).astype(jnp.float32)
    wanted = column(anchor_ref[...].astype(jnp.float32))
    member = (node_ids == wanted).astype(jnp.float32)
    inv_ref[...] = 1.0 / jnp.maximum(jnp.sum(member, axis=1, keepdims=True), 1.0)
    row = lax.broadcasted_iota(jnp.int32, (blocks, blocks), 0)
    moved = row == placed(me, count, (blocks, blocks), 1, blocks // count)
    moved = moved.astype(jnp.float32).astype(jnp.bfloat16)
    member_ref[...] = matmul(member.astype(jnp.bfloat16), moved).astype(jnp.bfloat16)
    there = placed(me, count, (anchors, nodes), 1, nodes_here).astype(jnp.float32)
    pick = (there == wanted).astype(jnp.float32).astype(jnp.bfloat16)
    asked_ref[...] = matmul(pick, held_ref[...])


def node_kernel(member_ref, inv_ref, asked_ref, pooled_ref, w_kv_ref, kv_ref):
    value = asked_ref[...] + matmul(member_ref[...], pooled_ref[...]) * inv_ref[...]
    mean = jnp.mean(value * value, axis=1, keepdims=True)
    feat = (value * lax.rsqrt(mean + 1e-06)).astype(jnp.bfloat16)
    kv_ref[...] = matmul(feat, w_kv_ref[...]).astype(jnp.bfloat16)


def attend(q_ref, kv_ref, out_ref, head_size):
    width, _ = q_ref.shape
    anchors = kv_ref.shape[0]
    pair = 2 * head_size
    lane = lax.broadcasted_iota(jnp.int32, (anchors, pair), 1)

    def score(j):
        at = slice(j * pair, (j + 1) * pair)
        keys = kv_ref[:, at]
        zero = jnp.zeros_like(keys)
        both = jnp.concatenate(
            [jnp.where(lane < head_size, keys, zero), jnp.where(lane >= head_size, keys, zero)], axis=0
        )
        return matmul(both, q_ref[at, :])

    def weigh(j, scores):
        values = kv_ref[:, width + j * pair : width + (j + 1) * pair].T
        ones = jnp.ones((HEAD_PAD, anchors), jnp.bfloat16)
        for h in range(2):
            part = scores[h * anchors : (h + 1) * anchors]
            part = jnp.exp2(part - jnp.max(part, axis=0, keepdims=True)).astype(jnp.bfloat16)
            left = jnp.concatenate([values[h * head_size : (h + 1) * head_size], ones], axis=0)
            got = matmul(left, part)
            got = got[:head_size] * (1.0 / got[head_size : head_size + 1])
            base = j * pair + h * head_size
            out_ref[base : base + head_size, :] = got.astype(jnp.bfloat16)

    ahead = score(0)
    for j in range(width // pair):
        scores = ahead
        if j + 1 < width // pair:
            ahead = score(j + 1)
        weigh(j, scores)


def self_kernel(q_ref, kv_ref, w_ref, out_ref, mid_ref, *, head_size):
    attend(q_ref, kv_ref, mid_ref, head_size)
    width = mid_ref.shape[0]
    out_ref[...] = matmul(mid_ref[...].T, w_ref[:width, :])


def cross_kernel(q_ref, kv_ref, w_ref, own_ref, out_ref, mid_ref, *, head_size):
    attend(q_ref, kv_ref, mid_ref, head_size)
    width = mid_ref.shape[0]
    out_ref[...] = (own_ref[...] + matmul(mid_ref[...].T, w_ref[width:, :])).astype(jnp.bfloat16)


def per_device(
    point_feat,
    query_feat,
    supernode_query,
    route_owner,
    route_slot,
    anchor_index,
    w_in,
    w_mid,
    w_q,
    w_kv,
    w_out,
):
    import functools

    head_size = D // HEADS
    shard_count = lax.axis_size("pts")
    points = point_feat[0]
    nblocks = points.shape[0] // BLK
    own = supernode_query[0]
    nodes_here, width = own.shape
    owners = route_owner.reshape(1, -1)
    blocks = owners.shape[1]
    nodes = nodes_here * shard_count
    anchors = anchor_index.shape[1]
    query_count = query_feat.shape[1]

    bits = masks(shard_count)
    rows = 2 * BLK
    log_e = 1.0 / math.log(2.0)

    def encode(points, begin, end, near):
        scratch = [
            pltpu.VMEM((2, rows, width), jnp.bfloat16),
            pltpu.VMEM(w_in.shape[1:], jnp.bfloat16),
        ]
        if not near:
            scratch += [
                pltpu.VMEM((end - begin, points.shape[1]), jnp.bfloat16),
                pltpu.VMEM(w_in.shape[1:], jnp.bfloat16),
                pltpu.VMEM(w_mid.shape[1:], jnp.bfloat16),
                pltpu.VMEM((end - begin, width), jnp.bfloat16),
                pltpu.SemaphoreType.DMA((4,)),
                pltpu.SemaphoreType.DMA(((end - begin) // rows,)),
            ]
        if near:
            return call(
                functools.partial(encode_kernel, base=begin, nodes_here=nodes_here),
                [shape((end - begin, width)), shape((nblocks, nodes))],
                scratch,
                flops=2 * (end - begin) * width * (width + points.shape[1]),
            )(points, w_in[0], w_mid[0], owners, route_slot)
        return call(
            functools.partial(encode_far_kernel, base=begin),
            shape((end - begin, width)),
            scratch,
            flops=2 * (end - begin) * width * (width + points.shape[1]),
            far=(0, 1, 2),
            far_out=True,
            limit=60 * MIB,
        )(points, w_in[0], w_mid[0])

    def pieces(stages):
        pairs = nblocks // 2
        cuts = [rows * (pairs * s // stages) for s in range(stages + 1)]
        cuts[1] -= 2 * rows
        return list(zip(cuts[:-1], cuts[1:]))

    stages = bits[:-2] + [bits[-2:]]
    held, encoded = own, []
    for stage, (begin, end) in zip(stages, pieces(len(stages))):
        last = isinstance(stage, list)
        got = [swapped(held, m) for m in (stage + [sum(stage)] if last else [stage])]
        done = encode(after(points, held) if encoded else points, begin, end, last)
        if last:
            done, mine = done
        encoded.append(done)
        got = [after(g, encoded[-1]) for g in got]
        held = jnp.concatenate([held] + got, axis=0)
    all_nodes = held
    pooled = call(
        functools.partial(pool_kernel, head_size=head_size),
        shape((nblocks, width)),
        [
            pltpu.VMEM((nblocks * HEAD_PAD, width), jnp.bfloat16),
            pltpu.VMEM((nblocks * HEAD_PAD, 2 * BLK), jnp.float32),
            pltpu.VMEM((nblocks * HEAD_PAD, 2 * BLK), jnp.bfloat16),
        ],
        flops=3e9,
    )(mine, all_nodes, *encoded)
    held = pooled
    for mask in bits[:-3]:
        held = jnp.concatenate([held, swapped(held, mask)], axis=0)
    up, right, down = bits[-3:]
    near = {m: swapped(held, m) for m in (up, right + down, right, down)}
    over = {m: swapped(near[up], m) for m in (right + down, right, down)}
    held = [held, near[up]]
    for m in (right, down, right + down):
        held += [near[m], over[m]]
    all_pooled = jnp.concatenate(held, axis=0)
    queries, asked, member, inv = call(
        functools.partial(query_kernel, scale=log_e / math.sqrt(head_size), nodes_here=nodes_here),
        [
            shape((width, query_count)),
            shape((anchors, width), jnp.float32),
            shape((anchors, blocks)),
            shape((anchors, 1), jnp.float32),
        ],
        flops=2 * query_count * width * width,
        limit=24 * MIB,
    )(owners, route_slot, anchor_index, after(all_nodes, pooled), query_feat[0], w_q[0])
    anchor_kv = call(node_kernel, shape((anchors, 2 * width)), flops=1e9)(
        member, inv, asked, all_pooled, w_kv[0]
    )
    partner_kv = lax.ppermute(anchor_kv, "branch", [(0, 1), (1, 0)])
    mid = [pltpu.VMEM((width, query_count), jnp.bfloat16)]
    self_part = call(
        functools.partial(self_kernel, head_size=head_size),
        shape((query_count, width), jnp.float32),
        mid,
        flops=3e9,
    )(queries, anchor_kv, w_out[0])
    result = call(
        functools.partial(cross_kernel, head_size=head_size),
        shape((query_count, width)),
        mid,
        flops=3e9,
    )(queries, partner_kv, w_out[0], self_part)
    return result[None]


def solution(mesh):
    return jax.shard_map(
        per_device,
        mesh=mesh,
        in_specs=(
            P("branch", ("groups", "pts"), None),
            P("branch", ("groups", "pts"), None),
            P("branch", ("groups", "pts"), None),
            P("branch", "groups", None),
            P("branch", "groups"),
            P("branch", "groups"),
            P("branch", None, None),
            P("branch", None, None),
            P("branch", None, None),
            P("branch", None, None),
            P("branch", None, None),
        ),
        out_specs=P("branch", ("groups", "pts"), None),
        check_vma=False,
    )
```
